32 devices in a mesh: groups: 2 (over y), gx: 16 (over z, x, core).
Axes of the slice: x: 2, y: 2, z: 4, core: 2. Of those that a mesh axis runs over, the one named last changes fastest.
Arguments:
- pressure: float32 [7, 256, 128, 128], P(None, ('groups', 'gx')), parts along dimension 1, may hold values from -6 to 6
- adjoint: float32 [7, 256, 128, 128], P(None, ('groups', 'gx')), parts along dimension 1, may hold values from -6 to 6
- permeability: float32 [3, 256, 128, 128], P(None, ('groups', 'gx')), parts along dimension 1, may hold values from 0.02 to 40, as said below
- active: int32 [256, 128, 128], P(('groups', 'gx')), parts along dimension 0, may hold values 0 or 1
- fault_codes: int32 [3, 256, 128, 128], P(None, ('groups', 'gx')), parts along dimension 1, may hold values from 0 to 3
Outputs:
- gradient: float32 [3, 256, 128, 128], P(None, ('groups', 'gx')), parts along dimension 1
The draws below stay inside these ranges and needn't reach their ends.
There are 2 independent parts, one for each index of `groups`. The reference program is written for one: setup_inputs(seed, part) draws one part's arguments, and reference() takes and returns one part's arrays. A program takes and returns all parts, laid end to end along the dimension named above; each array names one. Nothing has to cross between parts.
Inputs may be any that keep to these rules, and one draw needn't show every extreme that they name: `permeability`: Positive.
All inputs are finite; a program needn't handle non-finite values. No bound on the sum of `active` on one device may be relied on, other than what follows from the above.
Results may differ from the reference program's by a relative error of at most 0.0003.
Values sent between devices are 32-bit elements; how exact they have to be, the bound alone decides.
A program may use at most 64 MiB of HBM per device.

```python
import jax
import jax.numpy as jnp
from jax import lax

NT = 7
NY = 128
NZ = 128
NX = 128


def draw_permeability(key, part):
    shape = (3, NX, NY, NZ)
    position = jnp.arange(NX, dtype=jnp.float32) / NX
    rough = jnp.clip(0.7 * jax.random.normal(key, shape, jnp.float32), -2.1, 2.1)
    trend = 1.0 + 2.0 * position
    aniso = jnp.array([1.0, 1.0, 0.2], jnp.float32).reshape(3, 1, 1, 1)
    return (aniso * jnp.exp(rough) * trend[None, :, None, None]).astype(jnp.float32)


def plant(values, stream_key, least, high):
    longest = values.shape.index(max(values.shape))
    spots = []
    for shift in (0, 1):
        where = [jax.random.randint(jax.random.fold_in(stream_key, axis), (), 0, length) for axis, length in enumerate(values.shape)]
        where[longest] = (where[longest] + shift) % values.shape[longest]
        spots.append(tuple(where))
    return values.at[spots[0]].set(least).at[spots[1]].set(high)


def steps_of(rng, dims, split, least, high):
    level, own = 1.0, jax.random.fold_in(rng, 6)
    for axis_at, parts in split:
        steps = jnp.exp(jax.random.uniform(jax.random.fold_in(own, axis_at), (parts,), jnp.float32, least / len(split), high / len(split)))
        level = level * jnp.repeat(steps, dims[axis_at] // parts).reshape([-1 if axis == axis_at else 1 for axis in range(len(dims))])
    return level


def scatter_about(key, extent, width, reach, split=(), kind=jnp.bfloat16):
    drawn = jax.random.normal(key, extent, jnp.float32) * width
    if len(split) > 0:
        drawn = steps_of(key, extent, split, -0.22, 0.18) * drawn
    return jnp.clip(drawn, min=-reach, max=reach).astype(kind)


def setup_inputs(seed: int = 0, part: int = 0) -> dict:
    splits = jax.random.split(jax.random.key(seed), 6)
    part_splits = jax.random.split(jax.random.fold_in(splits[5], part), 6)
    return {
        "pressure": scatter_about(part_splits[0], (NT, NX, NY, NZ), 1.0, 6.0, ((1, 16),), jnp.float32),
        "adjoint": scatter_about(part_splits[1], (NT, NX, NY, NZ), 1.0, 6.0, ((1, 16),), jnp.float32),
        "permeability": draw_permeability(jax.random.fold_in(jax.random.fold_in(splits[5], part), 71), part),
        "active": plant((jax.random.randint(part_splits[3], (NX, NY, NZ), 0, 10) < 9).astype(jnp.int32), jax.random.fold_in(part_splits[3], 1), 0, 1),
        "fault_codes": plant(jax.random.randint(part_splits[4], (3, NX, NY, NZ), 0, 4), jax.random.fold_in(part_splits[4], 1), 0, 3).astype(jnp.int32),
    }


epsilon = 1e-06

def multiplier(codes):
    return jnp.where(codes == 0, 1.0, jnp.where(codes == 1, 0.6, jnp.where(codes == 2, 0.25, 0.05))).astype(jnp.float32)

def pair_terms(lower_pres, upper_pres, lower_adj, upper_adj, lower_perm, upper_perm, factor):
    products = lax.optimization_barrier(jnp.sum((lower_adj - upper_adj) * (lower_pres - upper_pres), axis=0))
    summed = lower_perm + upper_perm
    scaled = 2.0 * factor * products / (summed * summed)
    return (scaled * upper_perm * upper_perm, scaled * lower_perm * lower_perm)

def cut(values, start, stop, along):
    return lax.slice_in_dim(values, start, stop, axis=along)

def direction_grad(pressure, adjoint, perm_dir, opened, codes, along):
    count = opened.shape[along]
    factor = multiplier(cut(codes, 0, count - 1, along)) * cut(opened, 0, count - 1, along) * cut(opened, 1, count, along)
    to_lower, to_upper = pair_terms(cut(pressure, 0, count - 1, along + 1), cut(pressure, 1, count, along + 1), cut(adjoint, 0, count - 1, along + 1), cut(adjoint, 1, count, along + 1), cut(perm_dir, 0, count - 1, along), cut(perm_dir, 1, count, along), factor)
    widths_lower = [(0, 0), (0, 0), (0, 0)]
    widths_upper = [(0, 0), (0, 0), (0, 0)]
    widths_lower[along] = (0, 1)
    widths_upper[along] = (1, 0)
    return jnp.pad(to_lower, widths_lower) + jnp.pad(to_upper, widths_upper)

def reference(pressure, adjoint, permeability, active, fault_codes):
    opened = active.astype(jnp.float32)
    logs = []
    for direction in range(3):
        grad = direction_grad(pressure, adjoint, permeability[direction], opened, fault_codes[direction], direction)
        logs.append(permeability[direction] * grad)
    stacked = jnp.stack(logs)
    total = jnp.sum(stacked * stacked)
    root_mean = jnp.sqrt(total / (3 * NX * NY * NZ) + epsilon)
    return stacked / root_mean
```

```python
import functools

import jax
import jax.numpy as jnp
from jax import lax
from jax.experimental import pallas as pl
from jax.experimental.pallas import tpu as pltpu
from jax.sharding import PartitionSpec as P

MESH = pl.DeviceIdType.MESH
epsilon = 1e-06
ROWS = 64
CHUNK = 8
LATE = 4
PAD = 8
GRANT = 58_000_000


def doubled(codes):
    return jnp.where(codes == 0, 2.0, jnp.where(codes == 1, 1.2, jnp.where(codes == 2, 0.5, 0.1))).astype(jnp.float32)


def fold(values):
    squares = values * values
    total = squares[0:8]
    for i in range(8, squares.shape[0], 8):
        total = total + squares[i : i + 8]
    return total


def weight(products, factor, k_lo, k_up):
    summed = k_lo + k_up
    return factor * products * (k_lo * k_up) / jnp.maximum(summed * summed, 1e-30)


def distances(n):
    reach, rounds = 1, []
    while reach < n - 1:
        rounds.append(reach)
        reach *= 2
    return rounds


def down_shares(chips, chunks):
    return [max(chunks - (3 * chunks * q * q) // (4 * max(chips - 2, 1) ** 2), 0) for q in range(chips - 1)]


def kernel(
    n, p_hbm, a_hbm, k_hbm, act_hbm, code_hbm, grad, scale_out,
    pa, k, act, code, halo_t, halo_b, ret_t_out, ret_b_out, ret_t_in, ret_b_in, tail, part, parts,
    load_sem, chunk_recv, sems, near_sem,
):
    me = lax.axis_index("gx")
    lower, upper = me - 1, me + 1
    steps, layers, height, width = p_hbm.shape
    last = layers - 1
    blocks = height // ROWS
    chunks = height // CHUNK
    entries = 3 * layers * n * height * width
    K, FACTOR = 2 * steps, 2 * steps + 1
    OWN_UP, OWN_LO = 2 * steps + 1, 2 * steps + 2
    SEND, SEND_LATE, BACK_SEND, BACK, BACK_LATE, PAIR_SEND, PAIR, PAIR_BACK, PART_SEND, PART = range(10)

    odd = me % 2
    even = odd == 0
    odd = odd == 1
    has_lo, has_up = me > 0, me < n - 1
    apart = jnp.where(even, me, n - 1 - me) > 0
    chip = (me + 1) // 2 - 1
    shares = down_shares(n // 2, chunks)
    share = jnp.int32(0)
    for q, value in enumerate(shares):
        share = jnp.where(chip == q, value, share)
    share = jnp.where(apart, share, 0)
    rows_end = jnp.where(apart, chunks, 0)
    late_down = jnp.where(share > LATE, share - LATE, 0)
    late_up = jnp.where(rows_end - LATE > share, rows_end - LATE, share)

    def loop(start, stop, body):
        def step(i, carry):
            body(i)
            return carry

        lax.fori_loop(start, stop, step, 0)

    barrier = pltpu.get_barrier_semaphore()

    def signal(semaphore, distance):
        for there, inside in ((me - distance, me >= distance), (me + distance, me + distance < n)):
            @pl.when(inside)
            def _():
                pl.semaphore_signal(semaphore, inc=1, device_id={"gx": there}, device_id_type=MESH)

    def await_signals(semaphore, distance):
        peers = jnp.where(me >= distance, 1, 0) + jnp.where(me + distance < n, 1, 0)
        pl.semaphore_wait(semaphore, peers)

    signal(barrier, 1)
    rounds = distances(n)

    def turn(i):
        if i > 0:
            await_signals(near_sem.at[i - 1], rounds[i - 1])
        if i < len(rounds):
            signal(near_sem.at[i], rounds[i])

    def fields(l, sem):
        return (
            pltpu.make_async_copy(p_hbm.at[:, l], pa.at[pl.ds(0, steps), l, pl.ds(0, height)], sem),
            pltpu.make_async_copy(a_hbm.at[:, l], pa.at[pl.ds(steps, steps), l, pl.ds(0, height)], sem),
        )

    def cells(l, sem):
        return (
            pltpu.make_async_copy(k_hbm.at[:, l], k.at[:, l, pl.ds(0, height)], sem),
            pltpu.make_async_copy(act_hbm.at[l], act.at[l, pl.ds(0, height)], sem),
            pltpu.make_async_copy(code_hbm.at[:, l], code.at[:, l], sem),
        )

    def start_layer(l, sem):
        for copy in fields(l, sem) + cells(l, sem):
            copy.start()

    def await_planes(planes, rank, sem):
        ref = pa.at[pl.ds(0, planes), pl.ds(0, rank), pl.ds(0, height)]
        pltpu.make_async_copy(ref, ref, sem).wait()

    def layer_sem(l):
        return load_sem.at[l + 1]


    def chunk_rows(c):
        return pl.ds(pl.multiple_of(c * CHUNK, CHUNK), CHUNK)

    def down(c, planes, kind):
        rows = chunk_rows(c)
        return pltpu.make_async_remote_copy(
            src_ref=pa.at[pl.ds(0, planes), 0, rows], dst_ref=halo_t.at[pl.ds(0, planes), rows],
            send_sem=sems.at[kind], recv_sem=chunk_recv.at[c], device_id={"gx": lower}, device_id_type=MESH)

    def up(c, planes, kind):
        rows = chunk_rows(c)
        return pltpu.make_async_remote_copy(
            src_ref=pa.at[pl.ds(0, planes), last, rows], dst_ref=halo_b.at[pl.ds(0, planes), rows],
            send_sem=sems.at[kind], recv_sem=chunk_recv.at[c], device_id={"gx": upper}, device_id_type=MESH)

    def back_up(c, kind):
        rows = chunk_rows(c)
        return pltpu.make_async_remote_copy(
            src_ref=ret_t_out.at[rows], dst_ref=ret_b_in.at[rows],
            send_sem=sems.at[BACK_SEND], recv_sem=sems.at[kind], device_id={"gx": upper}, device_id_type=MESH)

    def back_down(c, kind):
        rows = chunk_rows(c)
        return pltpu.make_async_remote_copy(
            src_ref=ret_b_out.at[rows], dst_ref=ret_t_in.at[rows],
            send_sem=sems.at[BACK_SEND], recv_sem=sems.at[kind], device_id={"gx": lower}, device_id_type=MESH)

    D, DL, U, UL = 2 * steps + 1, 2 * steps + 2, 2 * steps + 2, 2 * steps + 3

    pair = pltpu.make_async_remote_copy(
        src_ref=pa.at[pl.ds(0, D), 0, pl.ds(0, height)], dst_ref=halo_t.at[pl.ds(0, D)],
        send_sem=sems.at[PAIR_SEND], recv_sem=sems.at[PAIR], device_id={"gx": lower}, device_id_type=MESH)
    pair_back = pltpu.make_async_remote_copy(
        src_ref=ret_t_out, dst_ref=ret_b_in,
        send_sem=sems.at[PAIR_SEND], recv_sem=sems.at[PAIR_BACK], device_id={"gx": upper}, device_id_type=MESH)

    def await_bytes(ref, sem):
        pltpu.make_async_copy(ref, ref, sems.at[sem]).wait()

    def await_rows(ref, count, sem):
        if count > 0:
            await_bytes(ref.at[pl.ds(0, count * CHUNK)], sem)

    def await_planes_of(ref, planes, count, sem):
        if count > 0:
            await_bytes(ref.at[pl.ds(0, planes), pl.ds(0, count * CHUNK)], sem)

    def each_share(side, body):
        for value in sorted(set(shares)):
            @pl.when(jnp.logical_and(jnp.logical_and(apart, side), share == value))
            def _(value=value):
                body(value, max(value - LATE, 0), max(chunks - LATE, value))

    for l in (0, last):
        for copy in fields(l, load_sem.at[0]):
            copy.start()
    pltpu.make_async_copy(k_hbm.at[0, last], pa.at[K, last, pl.ds(0, height)], load_sem.at[1]).start()
    for l in (0, last):
        for copy in cells(l, load_sem.at[1]):
            copy.start()

    tail[0:8] = jnp.zeros((8, width), jnp.float32)

    def clear(l):
        for t in range(2 * steps):
            pa[t, l, height:] = jnp.zeros((PAD, width), jnp.float32)
        k[1, l, height:] = jnp.zeros((PAD, width), jnp.float32)
        act[l, height:] = jnp.zeros((PAD, width), jnp.int32)

    loop(0, layers, clear)

    await_planes(2 * 7 + 1, 1, load_sem.at[1])
    pa[K, 0, 0:height] = k[0, 0, 0:height] * act[0, 0:height].astype(jnp.float32)
    pa[FACTOR, last, 0:height] = doubled(code[0, last]) * act[last, 0:height].astype(jnp.float32)
    await_planes(2 * steps, 2, load_sem.at[0])
    await_signals(barrier, 1)

    @pl.when(even)
    def _():
        loop(0, late_down, lambda c: down(c, D, SEND).start())

    @pl.when(odd)
    def _():
        loop(share, late_up, lambda c: up(c, U, SEND).start())
        pair.start()

    start_layer(1, load_sem.at[2])
    start_layer(last - 1, load_sem.at[2])
    loop(2, last - 1, lambda l: start_layer(l, layer_sem(l)))
    turn(0)

    zero = jnp.zeros((ROWS, width), jnp.float32)
    lane = lax.broadcasted_iota(jnp.int32, (ROWS, width), 1)
    for l in range(2, last - 1):
        grad[0, l] = jnp.zeros((height, width), jnp.float32)

    def opened(l, rows):
        return act[l, rows].astype(jnp.float32)

    def cross(l):
        def block(b):
            here = pl.ds(pl.multiple_of(b * ROWS, ROWS), ROWS)
            prod = zero
            for t in range(steps):
                prod += (pa[steps + t, l, here] - pa[steps + t, l + 1, here]) * (pa[t, l, here] - pa[t, l + 1, here])
            k0, k0_up = k[0, l, here] * opened(l, here), k[0, l + 1, here] * opened(l + 1, here)
            w = weight(prod, doubled(code[0, l, here]), k0, k0_up)
            grad[0, l, here] = w * k0_up
            grad[0, l + 1, here] = w * k0

        loop(0, blocks, block)

    await_planes(2 * steps, 3, load_sem.at[2])
    cross(0)
    cross(last - 1)
    pa[OWN_UP, 0, 0:height] = grad[0, 0]
    pa[OWN_LO, last, 0:height] = grad[0, last]

    @pl.when(even)
    def _():
        loop(late_down, share, lambda c: down(c, DL, SEND_LATE).start())

    @pl.when(odd)
    def _():
        loop(late_up, rows_end, lambda c: up(c, UL, SEND_LATE).start())

    def lanes_weight(l, r, prod):
        here = pl.ds(r, ROWS)
        k2 = k[2, l, here] * opened(l, here)
        k2_up = jnp.where(lane < width - 1, pltpu.roll(k2, width - 1, 1), 0.0)
        w = weight(prod, doubled(code[2, l, here]), k2, k2_up)
        return w * k2_up, w * k2

    def lanes_store(l, r, w_lo, w_up):
        log2 = w_lo + pltpu.roll(w_up, 1, 1)
        grad[2, l, pl.ds(r, ROWS)] = log2
        return fold(log2)

    def layer(l, carry, crossing):
        def block(b, carry):
            total, prod_z, w_lo, w_up, l1, r1, l2, r2 = carry
            r = pl.multiple_of(b * ROWS, ROWS)
            here, after = pl.ds(r, ROWS), pl.ds(r + 1, ROWS)
            total = total + lanes_store(l2, pl.multiple_of(r2, ROWS), w_lo, w_up)
            w_lo, w_up = lanes_weight(l1, pl.multiple_of(r1, ROWS), prod_z)
            prod_x, prod_y, prod_z = zero, zero, zero
            for t in range(steps):
                pt, at = pa[t, l, here], pa[steps + t, l, here]
                prod_z += (at - pltpu.roll(at, width - 1, 1)) * (pt - pltpu.roll(pt, width - 1, 1))
                prod_y += (at - pa[steps + t, l, after]) * (pt - pa[t, l, after])
                if crossing:
                    prod_x += (at - pa[steps + t, l + 1, here]) * (pt - pa[t, l + 1, here])
            now = opened(l, here)
            k1, k1_up = k[1, l, here] * now, k[1, l, after] * opened(l, after)
            w = weight(prod_y, doubled(code[1, l, here]), k1, k1_up)
            tail[pl.ds(r + 8, ROWS)] = w * k1
            log1 = w * k1_up + tail[pl.ds(r + 7, ROWS)]
            grad[1, l, here] = log1
            total = total + fold(log1)
            if crossing:
                k0, k0_up = k[0, l, here] * now, k[0, l + 1, here] * opened(l + 1, here)
                w = weight(prod_x, doubled(code[0, l, here]), k0, k0_up)
                log0 = grad[0, l, here] + w * k0_up
                grad[0, l, here] = log0
                grad[0, l + 1, here] = grad[0, l + 1, here] + w * k0
                total = total + fold(log0)
            return total, prod_z, w_lo, w_up, l, r, l1, r1

        return lax.fori_loop(0, blocks, block, carry)

    def border(i, carry):
        return layer(jnp.where(i == 0, 0, last + 1 - i), carry, False)

    def inner(l, carry):
        @pl.when(l < last - 2)
        def _():
            await_planes(steps, 3, layer_sem(l + 1))

        @pl.when(l == 2)
        def _():
            turn(1)

        return layer(l, carry, True)

    nothing = (jnp.zeros((8, width), jnp.float32), zero, zero, zero) + (jnp.int32(0),) * 4
    carry = lax.fori_loop(0, 3, border, nothing)
    total, prod_z, w_lo, w_up, l1, r1, l2, r2 = lax.fori_loop(1, last - 1, inner, carry)
    total = total + lanes_store(l2, pl.multiple_of(r2, ROWS), w_lo, w_up)
    w_lo, w_up = lanes_weight(l1, pl.multiple_of(r1, ROWS), prod_z)
    total = total + lanes_store(l1, pl.multiple_of(r1, ROWS), w_lo, w_up)
    total = total + fold(grad[0, last - 1])
    total = total + jnp.where(has_lo, 0.0, 1.0) * fold(grad[0, 0]) + jnp.where(has_up, 0.0, 1.0) * fold(grad[0, last])
    turn(2)

    def square(values):
        return values * values

    def face_top(rows, size):
        prod = jnp.zeros((size, width), jnp.float32)
        for t in range(steps):
            prod += (pa[steps + t, last, rows] - halo_t[steps + t, rows]) * (pa[t, last, rows] - halo_t[t, rows])
        k0, g_up = k[0, last, rows], halo_t[K, rows]
        w = weight(prod, pa[FACTOR, last, rows], k0, g_up)
        w_up = w * k0
        ret_t_out[rows] = w_up
        log0 = grad[0, last, rows] + w * g_up
        grad[0, last, rows] = log0
        return fold(log0), w_up

    def face_bottom(rows, size):
        prod = jnp.zeros((size, width), jnp.float32)
        for t in range(steps):
            prod += (halo_b[steps + t, rows] - pa[steps + t, 0, rows]) * (halo_b[t, rows] - pa[t, 0, rows])
        k0, g_up = halo_b[K, rows], pa[K, 0, rows]
        w = weight(prod, halo_b[FACTOR, rows], k0, g_up)
        w_lo = w * g_up
        ret_b_out[rows] = w_lo
        log0 = grad[0, 0, rows] + w * k0
        grad[0, 0, rows] = log0
        return fold(log0), w_lo

    def pair_face(b, total):
        squares, _ = face_top(pl.ds(pl.multiple_of(b * 32, 32), 32), 32)
        return total + squares

    @pl.when(even)
    def _():
        pair.wait_recv()

    total = lax.fori_loop(0, jnp.where(even, height // 32, 0), pair_face, total)

    @pl.when(even)
    def _():
        pair_back.start()

    def top_early(c, total):
        down(c, D, SEND).wait_recv()
        squares, _ = face_top(chunk_rows(c), CHUNK)
        back_up(c, BACK).start()
        return total + squares

    def top_late(c, total):
        down(c, DL, SEND_LATE).wait_recv()
        squares, w_up = face_top(chunk_rows(c), CHUNK)
        back_up(c, BACK_LATE).start()
        return total + squares + fold(halo_t[OWN_UP, chunk_rows(c)] + w_up)

    def bottom_early(c, total):
        up(c, U, SEND).wait_recv()
        squares, _ = face_bottom(chunk_rows(c), CHUNK)
        back_down(c, BACK).start()
        return total + squares

    def bottom_late(c, total):
        up(c, UL, SEND_LATE).wait_recv()
        squares, w_lo = face_bottom(chunk_rows(c), CHUNK)
        back_down(c, BACK_LATE).start()
        return total + squares + fold(halo_b[OWN_LO, chunk_rows(c)] + w_lo)

    def add_bottom(c, total):
        rows = chunk_rows(c)
        log0 = grad[0, 0, rows] + ret_b_in[rows]
        grad[0, 0, rows] = log0
        return total + fold(log0)

    def add_top(c, total):
        rows = chunk_rows(c)
        log0 = grad[0, last, rows] + ret_t_in[rows]
        grad[0, last, rows] = log0
        return total + fold(log0)

    def when_even(value):
        return jnp.where(even, value, 0)

    def when_odd(value):
        return jnp.where(odd, value, 0)

    @pl.when(odd)
    def _():
        pair_back.wait_recv()

    total = lax.fori_loop(0, when_odd(chunks), add_bottom, total)
    total = lax.fori_loop(0, when_odd(late_down), top_early, total)
    total = lax.fori_loop(when_even(share), when_even(late_up), bottom_early, total)
    for i in range(3, len(rounds)):
        turn(i)
    total = lax.fori_loop(when_odd(late_down), when_odd(share), top_late, total)
    total = lax.fori_loop(when_even(late_up), when_even(rows_end), bottom_late, total)
    each_share(even, lambda value, below, above: await_rows(ret_b_in, below, BACK))
    each_share(odd, lambda value, below, above: await_rows(ret_t_in, above - value, BACK))
    total = lax.fori_loop(0, when_even(late_down), add_bottom, total)
    total = lax.fori_loop(when_odd(share), when_odd(late_up), add_top, total)

    turn(len(rounds))
    mine = jnp.sum(total, axis=0, keepdims=True)
    part[...] = mine

    def to_peer(j):
        return pltpu.make_async_remote_copy(
            src_ref=part, dst_ref=parts.at[me], send_sem=sems.at[PART_SEND], recv_sem=sems.at[PART],
            device_id={"gx": j}, device_id_type=MESH)

    loop(0, me, lambda j: to_peer(j).start())
    loop(me + 1, n, lambda j: to_peer(j).start())
    parts[me] = mine

    each_share(even, lambda value, below, above: await_rows(ret_b_in, value - below, BACK_LATE))
    each_share(odd, lambda value, below, above: await_rows(ret_t_in, chunks - above, BACK_LATE))
    nowhere = jnp.zeros((8, width), jnp.float32)
    lax.fori_loop(when_even(late_down), when_even(share), add_bottom, nowhere)
    lax.fori_loop(when_odd(late_up), when_odd(rows_end), add_top, nowhere)

    def drain_even(value, below, above):
        await_planes_of(halo_t, D, below, SEND)
        await_planes_of(halo_t, DL, value - below, SEND_LATE)
        await_rows(ret_b_out, chunks - value, BACK_SEND)

    def drain_odd(value, below, above):
        await_planes_of(halo_b, U, above - value, SEND)
        await_planes_of(halo_b, UL, chunks - above, SEND_LATE)
        await_rows(ret_t_out, value, BACK_SEND)

    each_share(even, drain_even)
    each_share(odd, drain_odd)

    @pl.when(even)
    def _():
        pair_back.wait_send()

    @pl.when(odd)
    def _():
        pair.wait_send()

    others = parts.at[pl.ds(0, n - 1)]
    pltpu.make_async_copy(others, others, sems.at[PART_SEND]).wait()
    pltpu.make_async_copy(others, others, sems.at[PART]).wait()
    whole = jnp.sum(jnp.sum(parts[...], axis=0), keepdims=True)
    scale_out[...] = jnp.broadcast_to(lax.rsqrt(whole / entries + epsilon), scale_out.shape)


def finish(raw, scale, out, scaled, sem):
    dims, layers = raw.shape[:2]
    factor = jnp.broadcast_to(scale[0:1], raw.shape[2:])
    copies = []
    for l in range(layers):
        for d in range(dims):
            scaled[d, l] = raw[d, l] * factor
        copies.append(pltpu.make_async_copy(scaled.at[:, l], out.at[:, l], sem.at[l]))
        copies[-1].start()
    for copy in copies:
        copy.wait()


def local(pressure, adjoint, permeability, active, fault_codes):
    n = lax.axis_size("gx")
    steps, layers, height, width = pressure.shape
    chunks = height // CHUNK
    f32 = jnp.float32
    padded = height + PAD
    dma = pltpu.SemaphoreType.DMA
    raw, scale = pl.pallas_call(
        functools.partial(kernel, n),
        out_shape=(pltpu.VMEM((3, layers, height, width), f32), pltpu.VMEM((8, width), f32)),
        in_specs=[pl.BlockSpec(memory_space=pltpu.HBM)] * 5,
        out_specs=(pl.BlockSpec(memory_space=pltpu.VMEM), pl.BlockSpec(memory_space=pltpu.VMEM)),
        scratch_shapes=[
            pltpu.VMEM((2 * steps + 3, layers, padded, width), f32),
            pltpu.VMEM((3, layers, padded, width), f32),
            pltpu.VMEM((layers, padded, width), jnp.int32),
            pltpu.VMEM((3, layers, height, width), jnp.int32),
            pltpu.VMEM((2 * steps + 2, height, width), f32),
            pltpu.VMEM((2 * steps + 3, height, width), f32),
            pltpu.VMEM((height, width), f32),
            pltpu.VMEM((height, width), f32),
            pltpu.VMEM((height, width), f32),
            pltpu.VMEM((height, width), f32),
            pltpu.VMEM((padded, width), f32),
            pltpu.VMEM((1, width), f32),
            pltpu.VMEM((n, 1, width), f32),
            dma((layers - 1,)),
            dma((chunks,)),
            dma((10,)),
            pltpu.SemaphoreType.REGULAR((len(distances(n)),)),
        ],
        compiler_params=pltpu.CompilerParams(collective_id=0, has_side_effects=True, vmem_limit_bytes=GRANT),
        cost_estimate=pl.CostEstimate(flops=100_000_000, bytes_accessed=12_000_000, transcendentals=0),
        name="faces",
    )(pressure, adjoint, permeability, active, fault_codes)
    return pl.pallas_call(
        finish,
        out_shape=jax.ShapeDtypeStruct(raw.shape, f32),
        in_specs=[pl.BlockSpec(memory_space=pltpu.VMEM)] * 2,
        out_specs=pl.BlockSpec(memory_space=pltpu.HBM),
        scratch_shapes=[pltpu.VMEM((3, layers, height, width), f32), dma((layers,))],
        compiler_params=pltpu.CompilerParams(vmem_limit_bytes=8_000_000),
        name="finish",
    )(raw, scale)


def solution(mesh):
    split = ("groups", "gx")
    placed = (P(None, split), P(None, split), P(None, split), P(split), P(None, split))
    return jax.shard_map(local, mesh=mesh, in_specs=placed, out_specs=P(None, split), check_vma=False)
```

```python
import functools

import jax
import jax.numpy as jnp
from jax import lax
from jax.experimental import pallas as pl
from jax.experimental.pallas import tpu as pltpu
from jax.sharding import PartitionSpec as P

MESH = pl.DeviceIdType.MESH
epsilon = 1e-06
ROWS = 64
CHUNK = 8
LATE = 4
HEAD = 2
PAD = 8
GRANT = 58_000_000


def doubled(codes):
    return jnp.where(codes == 0, 2.0, jnp.where(codes == 1, 1.2, jnp.where(codes == 2, 0.5, 0.1))).astype(jnp.float32)


def fold(values):
    squares = values * values
    total = squares[0:8]
    for i in range(8, squares.shape[0], 8):
        total = total + squares[i : i + 8]
    return total


def weight(products, factor, k_lo, k_up):
    summed = k_lo + k_up
    return factor * products * (k_lo * k_up) / jnp.maximum(summed * summed, 1e-30)


def distances(n):
    reach, rounds = 1, []
    while reach < n - 1:
        rounds.append(reach)
        reach *= 2
    return rounds


def down_shares(chips, chunks):
    return [max(chunks - (3 * chunks * q * q) // (4 * max(chips - 2, 1) ** 2), 0) for q in range(chips - 1)]


def kernel(
    n, p_hbm, a_hbm, k_hbm, act_hbm, code_hbm, grad, scale_out,
    pa, k, act, code, halo_t, halo_b, ret_t_out, ret_b_out, ret_t_in, ret_b_in, tail, part, parts,
    load_sem, chunk_recv, sems, near_sem,
):
    me = lax.axis_index("gx")
    lower, upper = me - 1, me + 1
    steps, layers, height, width = p_hbm.shape
    last = layers - 1
    blocks = height // ROWS
    chunks = height // CHUNK
    entries = 3 * layers * n * height * width
    K, FACTOR = 2 * steps, 2 * steps + 1
    OWN_UP, OWN_LO = 2 * steps + 1, 2 * steps + 2
    SEND, SEND_LATE, BACK_SEND, BACK, BACK_LATE, PAIR_SEND, PAIR, PAIR_BACK, PART_SEND, PART = range(10)

    odd = me % 2
    even = odd == 0
    odd = odd == 1
    has_lo, has_up = me > 0, me < n - 1
    apart = jnp.where(even, me, n - 1 - me) > 0
    chip = (me + 1) // 2 - 1
    shares = down_shares(n // 2, chunks)
    share = jnp.int32(0)
    for q, value in enumerate(shares):
        share = jnp.where(chip == q, value, share)
    share = jnp.where(apart, share, 0)
    rows_end = jnp.where(apart, chunks, 0)
    late_down = jnp.where(share > LATE, share - LATE, 0)
    late_up = jnp.where(rows_end - LATE > share, rows_end - LATE, share)

    def loop(start, stop, body):
        def step(i, carry):
            body(i)
            return carry

        lax.fori_loop(start, stop, step, 0)

    barrier = pltpu.get_barrier_semaphore()

    def signal(semaphore, distance):
        for there, inside in ((me - distance, me >= distance), (me + distance, me + distance < n)):
            @pl.when(inside)
            def _():
                pl.semaphore_signal(semaphore, inc=1, device_id={"gx": there}, device_id_type=MESH)

    def await_signals(semaphore, distance):
        peers = jnp.where(me >= distance, 1, 0) + jnp.where(me + distance < n, 1, 0)
        pl.semaphore_wait(semaphore, peers)

    signal(barrier, 1)
    rounds = distances(n)

    def turn(i):
        if 0 < i <= len(rounds):
            await_signals(near_sem.at[i - 1], rounds[i - 1])
        if i < len(rounds):
            signal(near_sem.at[i], rounds[i])

    def fields(l, sem, start=0, stop=height):
        rows = pl.ds(start, stop - start)
        return (
            pltpu.make_async_copy(p_hbm.at[:, l, rows], pa.at[pl.ds(0, steps), l, rows], sem),
            pltpu.make_async_copy(a_hbm.at[:, l, rows], pa.at[pl.ds(steps, steps), l, rows], sem),
        )

    def k_of(start, stop, l, sem):
        axes = pl.ds(start, stop - start)
        return pltpu.make_async_copy(k_hbm.at[axes, l], k.at[axes, l, pl.ds(0, height)], sem)

    def code_of(start, stop, l, sem):
        axes = pl.ds(start, stop - start)
        return pltpu.make_async_copy(code_hbm.at[axes, l], code.at[axes, l], sem)

    def act_of(l, sem):
        return pltpu.make_async_copy(act_hbm.at[l], act.at[l, pl.ds(0, height)], sem)

    def cells(l, sem):
        return k_of(0, 3, l, sem), act_of(l, sem), code_of(0, 3, l, sem)

    def start_layer(l, sem):
        for copy in fields(l, sem) + cells(l, sem):
            copy.start()

    def await_planes(planes, rank, sem, rows=height):
        ref = pa.at[pl.ds(0, planes), pl.ds(0, rank), pl.ds(0, rows)]
        pltpu.make_async_copy(ref, ref, sem).wait()

    def layer_sem(l):
        return load_sem.at[l + 2]


    def chunk_rows(c):
        return pl.ds(pl.multiple_of(c * CHUNK, CHUNK), CHUNK)

    def down(c, planes, kind):
        rows = chunk_rows(c)
        return pltpu.make_async_remote_copy(
            src_ref=pa.at[pl.ds(0, planes), 0, rows], dst_ref=halo_t.at[pl.ds(0, planes), rows],
            send_sem=sems.at[kind], recv_sem=chunk_recv.at[c], device_id={"gx": lower}, device_id_type=MESH)

    def up(c, planes, kind):
        rows = chunk_rows(c)
        return pltpu.make_async_remote_copy(
            src_ref=pa.at[pl.ds(0, planes), last, rows], dst_ref=halo_b.at[pl.ds(0, planes), rows],
            send_sem=sems.at[kind], recv_sem=chunk_recv.at[c], device_id={"gx": upper}, device_id_type=MESH)

    def back_up(c, kind):
        rows = chunk_rows(c)
        return pltpu.make_async_remote_copy(
            src_ref=ret_t_out.at[rows], dst_ref=ret_b_in.at[rows],
            send_sem=sems.at[BACK_SEND], recv_sem=sems.at[kind], device_id={"gx": upper}, device_id_type=MESH)

    def back_down(c, kind):
        rows = chunk_rows(c)
        return pltpu.make_async_remote_copy(
            src_ref=ret_b_out.at[rows], dst_ref=ret_t_in.at[rows],
            send_sem=sems.at[BACK_SEND], recv_sem=sems.at[kind], device_id={"gx": lower}, device_id_type=MESH)

    D, DL, U, UL = 2 * steps + 1, 2 * steps + 2, 2 * steps + 2, 2 * steps + 3

    pair = pltpu.make_async_remote_copy(
        src_ref=pa.at[pl.ds(0, D), 0, pl.ds(0, height)], dst_ref=halo_t.at[pl.ds(0, D)],
        send_sem=sems.at[PAIR_SEND], recv_sem=sems.at[PAIR], device_id={"gx": lower}, device_id_type=MESH)
    pair_back = pltpu.make_async_remote_copy(
        src_ref=ret_t_out, dst_ref=ret_b_in,
        send_sem=sems.at[PAIR_SEND], recv_sem=sems.at[PAIR_BACK], device_id={"gx": upper}, device_id_type=MESH)

    def await_bytes(ref, sem):
        pltpu.make_async_copy(ref, ref, sems.at[sem]).wait()

    def await_rows(ref, count, sem):
        if count > 0:
            await_bytes(ref.at[pl.ds(0, count * CHUNK)], sem)

    def await_planes_of(ref, planes, count, sem):
        if count > 0:
            await_bytes(ref.at[pl.ds(0, planes), pl.ds(0, count * CHUNK)], sem)

    def each_share(side, body):
        for value in sorted(set(shares)):
            @pl.when(jnp.logical_and(jnp.logical_and(apart, side), share == value))
            def _(value=value):
                body(value, max(value - LATE, 0), max(chunks - LATE, value))

    head = HEAD * CHUNK
    load_k = pltpu.make_async_copy(k_hbm.at[0, last], pa.at[K, last, pl.ds(0, height)], load_sem.at[2])
    for copy in (
        (k_of(0, 1, 0, load_sem.at[0]), act_of(0, load_sem.at[0])) + fields(0, load_sem.at[0], 0, head)
        + fields(0, load_sem.at[1], head)
        + (load_k, act_of(last, load_sem.at[2]), code_of(0, 1, last, load_sem.at[2])) + fields(last, load_sem.at[2])
    ):
        copy.start()

    tail[0:8] = jnp.zeros((8, width), jnp.float32)

    def clear(l):
        for t in range(2 * steps):
            pa[t, l, height:] = jnp.zeros((PAD, width), jnp.float32)
        k[1, l, height:] = jnp.zeros((PAD, width), jnp.float32)
        act[l, height:] = jnp.zeros((PAD, width), jnp.int32)

    loop(0, layers, clear)

    await_signals(barrier, 1)
    await_planes(8, 1, load_sem.at[0], (2 * steps * head + 2 * height) // 8)
    pa[K, 0, 0:height] = k[0, 0, 0:height] * act[0, 0:height].astype(jnp.float32)
    ahead = jnp.where(late_down < HEAD, late_down, HEAD)

    @pl.when(even)
    def _():
        loop(0, ahead, lambda c: down(c, D, SEND).start())

    await_planes(2 * steps, 1, load_sem.at[1], height - head)

    @pl.when(even)
    def _():
        loop(ahead, late_down, lambda c: down(c, D, SEND).start())

    await_planes(2 * steps + 3, 1, load_sem.at[2])
    pa[FACTOR, last, 0:height] = doubled(code[0, last]) * act[last, 0:height].astype(jnp.float32)

    @pl.when(odd)
    def _():
        loop(share, late_up, lambda c: up(c, U, SEND).start())
        pair.start()

    for copy in (
        k_of(1, 3, 0, load_sem.at[3]), code_of(0, 3, 0, load_sem.at[3]),
        k_of(0, 3, last, load_sem.at[3]), code_of(1, 3, last, load_sem.at[3]),
    ):
        copy.start()
    start_layer(1, load_sem.at[3])
    start_layer(last - 1, load_sem.at[3])
    loop(2, last - 1, lambda l: start_layer(l, layer_sem(l)))
    turn(0)

    zero = jnp.zeros((ROWS, width), jnp.float32)
    lane = lax.broadcasted_iota(jnp.int32, (ROWS, width), 1)
    for l in range(2, last - 1):
        grad[0, l] = jnp.zeros((height, width), jnp.float32)

    def opened(l, rows):
        return act[l, rows].astype(jnp.float32)

    def cross(l):
        def block(b):
            here = pl.ds(pl.multiple_of(b * ROWS, ROWS), ROWS)
            prod = zero
            for t in range(steps):
                prod += (pa[steps + t, l, here] - pa[steps + t, l + 1, here]) * (pa[t, l, here] - pa[t, l + 1, here])
            k0, k0_up = k[0, l, here] * opened(l, here), k[0, l + 1, here] * opened(l + 1, here)
            w = weight(prod, doubled(code[0, l, here]), k0, k0_up)
            grad[0, l, here] = w * k0_up
            grad[0, l + 1, here] = w * k0

        loop(0, blocks, block)

    await_planes(2 * steps - 1, 4, load_sem.at[3])
    cross(0)
    cross(last - 1)
    turn(1)
    pa[OWN_UP, 0, 0:height] = grad[0, 0]
    pa[OWN_LO, last, 0:height] = grad[0, last]

    @pl.when(even)
    def _():
        loop(late_down, share, lambda c: down(c, DL, SEND_LATE).start())

    @pl.when(odd)
    def _():
        loop(late_up, rows_end, lambda c: up(c, UL, SEND_LATE).start())

    def lanes_weight(l, r, prod):
        here = pl.ds(r, ROWS)
        k2 = k[2, l, here] * opened(l, here)
        k2_up = jnp.where(lane < width - 1, pltpu.roll(k2, width - 1, 1), 0.0)
        w = weight(prod, doubled(code[2, l, here]), k2, k2_up)
        return w * k2_up, w * k2

    def lanes_store(l, r, w_lo, w_up):
        log2 = w_lo + pltpu.roll(w_up, 1, 1)
        grad[2, l, pl.ds(r, ROWS)] = log2
        return fold(log2)

    def layer(l, carry, crossing):
        def block(b, carry):
            total, prod_z, w_lo, w_up, l1, r1, l2, r2 = carry
            r = pl.multiple_of(b * ROWS, ROWS)
            here, after = pl.ds(r, ROWS), pl.ds(r + 1, ROWS)
            total = total + lanes_store(l2, pl.multiple_of(r2, ROWS), w_lo, w_up)
            w_lo, w_up = lanes_weight(l1, pl.multiple_of(r1, ROWS), prod_z)
            prod_x, prod_y, prod_z = zero, zero, zero
            for t in range(steps):
                pt, at = pa[t, l, here], pa[steps + t, l, here]
                prod_z += (at - pltpu.roll(at, width - 1, 1)) * (pt - pltpu.roll(pt, width - 1, 1))
                prod_y += (at - pa[steps + t, l, after]) * (pt - pa[t, l, after])
                if crossing:
                    prod_x += (at - pa[steps + t, l + 1, here]) * (pt - pa[t, l + 1, here])
            now = opened(l, here)
            k1, k1_up = k[1, l, here] * now, k[1, l, after] * opened(l, after)
            w = weight(prod_y, doubled(code[1, l, here]), k1, k1_up)
            tail[pl.ds(r + 8, ROWS)] = w * k1
            log1 = w * k1_up + tail[pl.ds(r + 7, ROWS)]
            grad[1, l, here] = log1
            total = total + fold(log1)
            if crossing:
                k0, k0_up = k[0, l, here] * now, k[0, l + 1, here] * opened(l + 1, here)
                w = weight(prod_x, doubled(code[0, l, here]), k0, k0_up)
                log0 = grad[0, l, here] + w * k0_up
                grad[0, l, here] = log0
                grad[0, l + 1, here] = grad[0, l + 1, here] + w * k0
                total = total + fold(log0)
            return total, prod_z, w_lo, w_up, l, r, l1, r1

        return lax.fori_loop(0, blocks, block, carry)

    def border(i, carry):
        return layer(jnp.where(i == 0, 0, last + 1 - i), carry, False)

    def inner(l, carry):
        @pl.when(l < last - 2)
        def _():
            await_planes(steps, 3, layer_sem(l + 1))

        for i, at_layer in ((2, 1), (3, last - 3)):
            @pl.when(l == at_layer)
            def _(i=i):
                turn(i)

        return layer(l, carry, True)

    nothing = (jnp.zeros((8, width), jnp.float32), zero, zero, zero) + (jnp.int32(0),) * 4
    carry = lax.fori_loop(0, 3, border, nothing)
    total, prod_z, w_lo, w_up, l1, r1, l2, r2 = lax.fori_loop(1, last - 1, inner, carry)
    total = total + lanes_store(l2, pl.multiple_of(r2, ROWS), w_lo, w_up)
    w_lo, w_up = lanes_weight(l1, pl.multiple_of(r1, ROWS), prod_z)
    total = total + lanes_store(l1, pl.multiple_of(r1, ROWS), w_lo, w_up)
    total = total + fold(grad[0, last - 1])
    total = total + jnp.where(has_lo, 0.0, 1.0) * fold(grad[0, 0]) + jnp.where(has_up, 0.0, 1.0) * fold(grad[0, last])
    def square(values):
        return values * values

    def face_top(rows, size):
        prod = jnp.zeros((size, width), jnp.float32)
        for t in range(steps):
            prod += (pa[steps + t, last, rows] - halo_t[steps + t, rows]) * (pa[t, last, rows] - halo_t[t, rows])
        k0, g_up = k[0, last, rows], halo_t[K, rows]
        w = weight(prod, pa[FACTOR, last, rows], k0, g_up)
        w_up = w * k0
        ret_t_out[rows] = w_up
        log0 = grad[0, last, rows] + w * g_up
        grad[0, last, rows] = log0
        return fold(log0), w_up

    def face_bottom(rows, size):
        prod = jnp.zeros((size, width), jnp.float32)
        for t in range(steps):
            prod += (halo_b[steps + t, rows] - pa[steps + t, 0, rows]) * (halo_b[t, rows] - pa[t, 0, rows])
        k0, g_up = halo_b[K, rows], pa[K, 0, rows]
        w = weight(prod, halo_b[FACTOR, rows], k0, g_up)
        w_lo = w * g_up
        ret_b_out[rows] = w_lo
        log0 = grad[0, 0, rows] + w * k0
        grad[0, 0, rows] = log0
        return fold(log0), w_lo

    def pair_face(b, total):
        squares, _ = face_top(pl.ds(pl.multiple_of(b * 32, 32), 32), 32)
        return total + squares

    @pl.when(even)
    def _():
        pair.wait_recv()

    total = lax.fori_loop(0, jnp.where(even, height // 32, 0), pair_face, total)

    @pl.when(even)
    def _():
        pair_back.start()

    def top_early(c, total):
        down(c, D, SEND).wait_recv()
        squares, _ = face_top(chunk_rows(c), CHUNK)
        back_up(c, BACK).start()
        return total + squares

    def top_late(c, total):
        down(c, DL, SEND_LATE).wait_recv()
        squares, w_up = face_top(chunk_rows(c), CHUNK)
        back_up(c, BACK_LATE).start()
        return total + squares + fold(halo_t[OWN_UP, chunk_rows(c)] + w_up)

    def bottom_early(c, total):
        up(c, U, SEND).wait_recv()
        squares, _ = face_bottom(chunk_rows(c), CHUNK)
        back_down(c, BACK).start()
        return total + squares

    def bottom_late(c, total):
        up(c, UL, SEND_LATE).wait_recv()
        squares, w_lo = face_bottom(chunk_rows(c), CHUNK)
        back_down(c, BACK_LATE).start()
        return total + squares + fold(halo_b[OWN_LO, chunk_rows(c)] + w_lo)

    def add_bottom(c, total):
        rows = chunk_rows(c)
        log0 = grad[0, 0, rows] + ret_b_in[rows]
        grad[0, 0, rows] = log0
        return total + fold(log0)

    def add_top(c, total):
        rows = chunk_rows(c)
        log0 = grad[0, last, rows] + ret_t_in[rows]
        grad[0, last, rows] = log0
        return total + fold(log0)

    def when_even(value):
        return jnp.where(even, value, 0)

    def when_odd(value):
        return jnp.where(odd, value, 0)

    @pl.when(odd)
    def _():
        pair_back.wait_recv()

    total = lax.fori_loop(0, when_odd(chunks), add_bottom, total)
    total = lax.fori_loop(0, when_odd(late_down), top_early, total)
    total = lax.fori_loop(when_even(share), when_even(late_up), bottom_early, total)
    for i in range(4, len(rounds) + 1):
        turn(i)
    each_share(even, lambda value, below, above: await_rows(ret_b_in, below, BACK))
    each_share(odd, lambda value, below, above: await_rows(ret_t_in, above - value, BACK))
    total = lax.fori_loop(0, when_even(late_down), add_bottom, total)
    total = lax.fori_loop(when_odd(share), when_odd(late_up), add_top, total)
    total = lax.fori_loop(when_odd(late_down), when_odd(share), top_late, total)
    total = lax.fori_loop(when_even(late_up), when_even(rows_end), bottom_late, total)

    mine = jnp.sum(total, axis=0, keepdims=True)
    part[...] = mine

    def to_peer(j):
        return pltpu.make_async_remote_copy(
            src_ref=part, dst_ref=parts.at[me], send_sem=sems.at[PART_SEND], recv_sem=sems.at[PART],
            device_id={"gx": j}, device_id_type=MESH)

    loop(0, me, lambda j: to_peer(j).start())
    loop(me + 1, n, lambda j: to_peer(j).start())
    parts[me] = mine

    each_share(even, lambda value, below, above: await_rows(ret_b_in, value - below, BACK_LATE))
    each_share(odd, lambda value, below, above: await_rows(ret_t_in, chunks - above, BACK_LATE))
    nowhere = jnp.zeros((8, width), jnp.float32)
    lax.fori_loop(when_even(late_down), when_even(share), add_bottom, nowhere)
    lax.fori_loop(when_odd(late_up), when_odd(rows_end), add_top, nowhere)

    def drain_even(value, below, above):
        await_planes_of(halo_t, D, below, SEND)
        await_planes_of(halo_t, DL, value - below, SEND_LATE)
        await_rows(ret_b_out, chunks - value, BACK_SEND)

    def drain_odd(value, below, above):
        await_planes_of(halo_b, U, above - value, SEND)
        await_planes_of(halo_b, UL, chunks - above, SEND_LATE)
        await_rows(ret_t_out, value, BACK_SEND)

    each_share(even, drain_even)
    each_share(odd, drain_odd)

    @pl.when(even)
    def _():
        pair_back.wait_send()

    @pl.when(odd)
    def _():
        pair.wait_send()

    others = parts.at[pl.ds(0, n - 1)]
    pltpu.make_async_copy(others, others, sems.at[PART_SEND]).wait()
    pltpu.make_async_copy(others, others, sems.at[PART]).wait()
    whole = jnp.sum(jnp.sum(parts[...], axis=0), keepdims=True)
    scale_out[...] = jnp.broadcast_to(lax.rsqrt(whole / entries + epsilon), scale_out.shape)


def finish(raw, scale, out, scaled, sem):
    dims, layers = raw.shape[:2]
    factor = jnp.broadcast_to(scale[0:1], raw.shape[2:])
    for d in range(dims):
        for l in range(layers):
            scaled[d, l] = raw[d, l] * factor
            pltpu.make_async_copy(scaled.at[d, l], out.at[d, l], sem.at[0]).start()
    pltpu.make_async_copy(scaled, out, sem.at[0]).wait()


def local(pressure, adjoint, permeability, active, fault_codes):
    n = lax.axis_size("gx")
    steps, layers, height, width = pressure.shape
    chunks = height // CHUNK
    f32 = jnp.float32
    padded = height + PAD
    dma = pltpu.SemaphoreType.DMA
    raw, scale = pl.pallas_call(
        functools.partial(kernel, n),
        out_shape=(pltpu.VMEM((3, layers, height, width), f32), pltpu.VMEM((8, width), f32)),
        in_specs=[pl.BlockSpec(memory_space=pltpu.HBM)] * 5,
        out_specs=(pl.BlockSpec(memory_space=pltpu.VMEM), pl.BlockSpec(memory_space=pltpu.VMEM)),
        scratch_shapes=[
            pltpu.VMEM((2 * steps + 3, layers, padded, width), f32),
            pltpu.VMEM((3, layers, padded, width), f32),
            pltpu.VMEM((layers, padded, width), jnp.int32),
            pltpu.VMEM((3, layers, height, width), jnp.int32),
            pltpu.VMEM((2 * steps + 2, height, width), f32),
            pltpu.VMEM((2 * steps + 3, height, width), f32),
            pltpu.VMEM((height, width), f32),
            pltpu.VMEM((height, width), f32),
            pltpu.VMEM((height, width), f32),
            pltpu.VMEM((height, width), f32),
            pltpu.VMEM((padded, width), f32),
            pltpu.VMEM((1, width), f32),
            pltpu.VMEM((n, 1, width), f32),
            dma((layers,)),
            dma((chunks,)),
            dma((10,)),
            pltpu.SemaphoreType.REGULAR((len(distances(n)),)),
        ],
        compiler_params=pltpu.CompilerParams(collective_id=0, has_side_effects=True, vmem_limit_bytes=GRANT),
        cost_estimate=pl.CostEstimate(flops=100_000_000, bytes_accessed=12_000_000, transcendentals=0),
        name="faces",
    )(pressure, adjoint, permeability, active, fault_codes)
    return pl.pallas_call(
        finish,
        out_shape=jax.ShapeDtypeStruct(raw.shape, f32),
        in_specs=[pl.BlockSpec(memory_space=pltpu.VMEM)] * 2,
        out_specs=pl.BlockSpec(memory_space=pltpu.HBM),
        scratch_shapes=[pltpu.VMEM((3, layers, height, width), f32), dma((1,))],
        compiler_params=pltpu.CompilerParams(vmem_limit_bytes=8_000_000),
        name="finish",
    )(raw, scale)


def solution(mesh):
    split = ("groups", "gx")
    placed = (P(None, split), P(None, split), P(None, split), P(split), P(None, split))
    return jax.shard_map(local, mesh=mesh, in_specs=placed, out_specs=P(None, split), check_vma=False)
```

```python
import functools

import jax
import jax.numpy as jnp
from jax import lax
from jax.experimental import pallas as pl
from jax.experimental.pallas import tpu as pltpu
from jax.sharding import PartitionSpec as P

MESH = pl.DeviceIdType.MESH
epsilon = 1e-06
ROWS = 64
CHUNK = 8
LATE = 4
HEAD = 2
PAD = 8
GRANT = 58_000_000


def doubled(codes):
    return jnp.where(codes == 0, 2.0, jnp.where(codes == 1, 1.2, jnp.where(codes == 2, 0.5, 0.1))).astype(jnp.float32)


def fold(values):
    squares = values * values
    total = squares[0:8]
    for i in range(8, squares.shape[0], 8):
        total = total + squares[i : i + 8]
    return total


def weight(products, factor, k_lo, k_up):
    summed = k_lo + k_up
    return factor * products * (k_lo * k_up) / jnp.maximum(summed * summed, 1e-30)


def distances(n):
    reach, rounds = 1, []
    while reach < n - 1:
        rounds.append(reach)
        reach *= 2
    return rounds


def down_shares(chips, chunks):
    rise = [(3 * chunks * q * q) // (4 * max(chips - 2, 1) ** 2) for q in range(chips - 1)]
    return [chunks - min(max(up, min(q, 1)), chunks) for q, up in enumerate(rise)]


def kernel(
    n, p_hbm, a_hbm, k_hbm, act_hbm, code_hbm, grad, scale_out,
    pa, k, act, code, halo_t, halo_b, ret_t_out, ret_b_out, ret_t_in, ret_b_in, tail, part, parts,
    load_sem, chunk_recv, sems, near_sem,
):
    me = lax.axis_index("gx")
    lower, upper = me - 1, me + 1
    steps, layers, height, width = p_hbm.shape
    last = layers - 1
    blocks = height // ROWS
    chunks = height // CHUNK
    entries = 3 * layers * n * height * width
    K, FACTOR = 2 * steps, 2 * steps + 1
    OWN_UP, OWN_LO = 2 * steps + 1, 2 * steps + 2
    SEND, SEND_LATE, BACK_SEND, BACK, BACK_LATE, PAIR_SEND, PAIR, PAIR_BACK, PART_SEND, PART = range(10)

    odd = me % 2
    even = odd == 0
    odd = odd == 1
    has_lo, has_up = me > 0, me < n - 1
    apart = jnp.where(even, me, n - 1 - me) > 0
    chip = (me + 1) // 2 - 1
    shares = down_shares(n // 2, chunks)
    share = jnp.int32(0)
    for q, value in enumerate(shares):
        share = jnp.where(chip == q, value, share)
    share = jnp.where(apart, share, 0)
    rows_end = jnp.where(apart, chunks, 0)
    late_down = jnp.where(share > LATE, share - LATE, 0)
    late_up = jnp.where(rows_end - LATE > share, rows_end - LATE, share)

    def loop(start, stop, body):
        def step(i, carry):
            body(i)
            return carry

        lax.fori_loop(start, stop, step, 0)

    barrier = pltpu.get_barrier_semaphore()

    def signal(semaphore, distance):
        for there, inside in ((me - distance, me >= distance), (me + distance, me + distance < n)):
            @pl.when(inside)
            def _():
                pl.semaphore_signal(semaphore, inc=1, device_id={"gx": there}, device_id_type=MESH)

    def await_signals(semaphore, distance):
        peers = jnp.where(me >= distance, 1, 0) + jnp.where(me + distance < n, 1, 0)
        pl.semaphore_wait(semaphore, peers)

    def fields(l, sem, start=0, stop=height):
        rows = pl.ds(start, stop - start)
        return (
            pltpu.make_async_copy(p_hbm.at[:, l, rows], pa.at[pl.ds(0, steps), l, rows], sem),
            pltpu.make_async_copy(a_hbm.at[:, l, rows], pa.at[pl.ds(steps, steps), l, rows], sem),
        )

    def k_of(start, stop, l, sem):
        axes = pl.ds(start, stop - start)
        return pltpu.make_async_copy(k_hbm.at[axes, l], k.at[axes, l, pl.ds(0, height)], sem)

    def code_of(start, stop, l, sem):
        axes = pl.ds(start, stop - start)
        return pltpu.make_async_copy(code_hbm.at[axes, l], code.at[axes, l], sem)

    def act_of(l, sem):
        return pltpu.make_async_copy(act_hbm.at[l], act.at[l, pl.ds(0, height)], sem)

    def cells(l, sem):
        return k_of(0, 3, l, sem), act_of(l, sem), code_of(0, 3, l, sem)

    head = HEAD * CHUNK
    load_k = pltpu.make_async_copy(k_hbm.at[0, last], pa.at[K, last, pl.ds(0, height)], load_sem.at[2])
    for copy in (
        (k_of(0, 1, 0, load_sem.at[0]), act_of(0, load_sem.at[0])) + fields(0, load_sem.at[0], 0, head)
        + fields(0, load_sem.at[1], head)
        + (load_k, act_of(last, load_sem.at[2]), code_of(0, 1, last, load_sem.at[2])) + fields(last, load_sem.at[2])
    ):
        copy.start()

    signal(barrier, 1)
    rounds = distances(n)

    def turn(i):
        if 0 < i <= len(rounds):
            await_signals(near_sem.at[i - 1], rounds[i - 1])
        if i < len(rounds):
            signal(near_sem.at[i], rounds[i])

    def start_layer(l, sem):
        for copy in fields(l, sem) + cells(l, sem):
            copy.start()

    def await_planes(planes, rank, sem, rows=height):
        ref = pa.at[pl.ds(0, planes), pl.ds(0, rank), pl.ds(0, rows)]
        pltpu.make_async_copy(ref, ref, sem).wait()

    def layer_sem(l):
        return load_sem.at[l + 2]


    def chunk_rows(c):
        return pl.ds(pl.multiple_of(c * CHUNK, CHUNK), CHUNK)

    def down(c, planes, kind):
        rows = chunk_rows(c)
        return pltpu.make_async_remote_copy(
            src_ref=pa.at[pl.ds(0, planes), 0, rows], dst_ref=halo_t.at[pl.ds(0, planes), rows],
            send_sem=sems.at[kind], recv_sem=chunk_recv.at[c], device_id={"gx": lower}, device_id_type=MESH)

    def up(c, planes, kind):
        rows = chunk_rows(c)
        return pltpu.make_async_remote_copy(
            src_ref=pa.at[pl.ds(0, planes), last, rows], dst_ref=halo_b.at[pl.ds(0, planes), rows],
            send_sem=sems.at[kind], recv_sem=chunk_recv.at[c], device_id={"gx": upper}, device_id_type=MESH)

    def back_up(c, kind):
        rows = chunk_rows(c)
        return pltpu.make_async_remote_copy(
            src_ref=ret_t_out.at[rows], dst_ref=ret_b_in.at[rows],
            send_sem=sems.at[BACK_SEND], recv_sem=sems.at[kind], device_id={"gx": upper}, device_id_type=MESH)

    def back_down(c, kind):
        rows = chunk_rows(c)
        return pltpu.make_async_remote_copy(
            src_ref=ret_b_out.at[rows], dst_ref=ret_t_in.at[rows],
            send_sem=sems.at[BACK_SEND], recv_sem=sems.at[kind], device_id={"gx": lower}, device_id_type=MESH)

    D, DL, U, UL = 2 * steps + 1, 2 * steps + 2, 2 * steps + 2, 2 * steps + 3

    pair = pltpu.make_async_remote_copy(
        src_ref=pa.at[pl.ds(0, D), 0, pl.ds(0, height)], dst_ref=halo_t.at[pl.ds(0, D)],
        send_sem=sems.at[PAIR_SEND], recv_sem=sems.at[PAIR], device_id={"gx": lower}, device_id_type=MESH)
    pair_back = pltpu.make_async_remote_copy(
        src_ref=ret_t_out, dst_ref=ret_b_in,
        send_sem=sems.at[PAIR_SEND], recv_sem=sems.at[PAIR_BACK], device_id={"gx": upper}, device_id_type=MESH)

    def await_bytes(ref, sem):
        pltpu.make_async_copy(ref, ref, sems.at[sem]).wait()

    def await_rows(ref, count, sem):
        if count > 0:
            await_bytes(ref.at[pl.ds(0, count * CHUNK)], sem)

    def await_planes_of(ref, planes, count, sem):
        if count > 0:
            await_bytes(ref.at[pl.ds(0, planes), pl.ds(0, count * CHUNK)], sem)

    def each_share(side, body):
        for value in sorted(set(shares)):
            @pl.when(jnp.logical_and(jnp.logical_and(apart, side), share == value))
            def _(value=value):
                body(value, max(value - LATE, 0), max(chunks - LATE, value))

    tail[0:8] = jnp.zeros((8, width), jnp.float32)

    def clear(l):
        for t in range(2 * steps):
            pa[t, l, height:] = jnp.zeros((PAD, width), jnp.float32)
        k[1, l, height:] = jnp.zeros((PAD, width), jnp.float32)
        act[l, height:] = jnp.zeros((PAD, width), jnp.int32)

    loop(0, layers, clear)

    await_signals(barrier, 1)
    await_planes(8, 1, load_sem.at[0], (2 * steps * head + 2 * height) // 8)
    pa[K, 0, 0:height] = k[0, 0, 0:height] * act[0, 0:height].astype(jnp.float32)
    ahead = jnp.where(late_down < HEAD, late_down, HEAD)

    @pl.when(even)
    def _():
        loop(0, ahead, lambda c: down(c, D, SEND).start())

    await_planes(2 * steps, 1, load_sem.at[1], height - head)

    @pl.when(even)
    def _():
        loop(ahead, late_down, lambda c: down(c, D, SEND).start())

    await_planes(2 * steps + 3, 1, load_sem.at[2])
    pa[FACTOR, last, 0:height] = doubled(code[0, last]) * act[last, 0:height].astype(jnp.float32)

    @pl.when(odd)
    def _():
        loop(share, late_up, lambda c: up(c, U, SEND).start())
        pair.start()

    for copy in (
        k_of(1, 3, 0, load_sem.at[3]), code_of(0, 3, 0, load_sem.at[3]),
        k_of(0, 3, last, load_sem.at[3]), code_of(1, 3, last, load_sem.at[3]),
    ):
        copy.start()
    start_layer(1, load_sem.at[3])
    start_layer(last - 1, load_sem.at[3])
    loop(2, last - 1, lambda l: start_layer(l, layer_sem(l)))
    turn(0)

    zero = jnp.zeros((ROWS, width), jnp.float32)
    lane = lax.broadcasted_iota(jnp.int32, (ROWS, width), 1)
    for l in range(2, last - 1):
        grad[0, l] = jnp.zeros((height, width), jnp.float32)

    def opened(l, rows):
        return act[l, rows].astype(jnp.float32)

    def cross(l):
        def block(b):
            here = pl.ds(pl.multiple_of(b * ROWS, ROWS), ROWS)
            prod = zero
            for t in range(steps):
                prod += (pa[steps + t, l, here] - pa[steps + t, l + 1, here]) * (pa[t, l, here] - pa[t, l + 1, here])
            k0, k0_up = k[0, l, here] * opened(l, here), k[0, l + 1, here] * opened(l + 1, here)
            w = weight(prod, doubled(code[0, l, here]), k0, k0_up)
            grad[0, l, here] = w * k0_up
            grad[0, l + 1, here] = w * k0

        loop(0, blocks, block)

    await_planes(2 * steps - 1, 4, load_sem.at[3])
    cross(0)
    cross(last - 1)
    turn(1)
    pa[OWN_UP, 0, 0:height] = grad[0, 0]
    pa[OWN_LO, last, 0:height] = grad[0, last]

    @pl.when(even)
    def _():
        loop(late_down, share, lambda c: down(c, DL, SEND_LATE).start())

    @pl.when(odd)
    def _():
        loop(late_up, rows_end, lambda c: up(c, UL, SEND_LATE).start())

    def lanes_weight(l, r, prod):
        here = pl.ds(r, ROWS)
        k2 = k[2, l, here] * opened(l, here)
        k2_up = jnp.where(lane < width - 1, pltpu.roll(k2, width - 1, 1), 0.0)
        w = weight(prod, doubled(code[2, l, here]), k2, k2_up)
        return w * k2_up, w * k2

    def lanes_store(l, r, w_lo, w_up):
        log2 = w_lo + pltpu.roll(w_up, 1, 1)
        grad[2, l, pl.ds(r, ROWS)] = log2
        return fold(log2)

    def layer(l, carry, crossing):
        def block(b, carry):
            total, prod_z, w_lo, w_up, l1, r1, l2, r2 = carry
            r = pl.multiple_of(b * ROWS, ROWS)
            here, after = pl.ds(r, ROWS), pl.ds(r + 1, ROWS)
            total = total + lanes_store(l2, pl.multiple_of(r2, ROWS), w_lo, w_up)
            w_lo, w_up = lanes_weight(l1, pl.multiple_of(r1, ROWS), prod_z)
            prod_x, prod_y, prod_z = zero, zero, zero
            for t in range(steps):
                pt, at = pa[t, l, here], pa[steps + t, l, here]
                prod_z += (at - pltpu.roll(at, width - 1, 1)) * (pt - pltpu.roll(pt, width - 1, 1))
                prod_y += (at - pa[steps + t, l, after]) * (pt - pa[t, l, after])
                if crossing:
                    prod_x += (at - pa[steps + t, l + 1, here]) * (pt - pa[t, l + 1, here])
            now = opened(l, here)
            k1, k1_up = k[1, l, here] * now, k[1, l, after] * opened(l, after)
            w = weight(prod_y, doubled(code[1, l, here]), k1, k1_up)
            tail[pl.ds(r + 8, ROWS)] = w * k1
            log1 = w * k1_up + tail[pl.ds(r + 7, ROWS)]
            grad[1, l, here] = log1
            total = total + fold(log1)
            if crossing:
                k0, k0_up = k[0, l, here] * now, k[0, l + 1, here] * opened(l + 1, here)
                w = weight(prod_x, doubled(code[0, l, here]), k0, k0_up)
                log0 = grad[0, l, here] + w * k0_up
                grad[0, l, here] = log0
                grad[0, l + 1, here] = grad[0, l + 1, here] + w * k0
                total = total + fold(log0)
            return total, prod_z, w_lo, w_up, l, r, l1, r1

        return lax.fori_loop(0, blocks, block, carry)

    def border(i, carry):
        return layer(jnp.where(i == 0, 0, last + 1 - i), carry, False)

    def inner(l, carry):
        @pl.when(l < last - 2)
        def _():
            await_planes(steps, 3, layer_sem(l + 1))

        for i, at_layer in ((2, 1), (3, last - 3)):
            @pl.when(l == at_layer)
            def _(i=i):
                turn(i)

        return layer(l, carry, True)

    nothing = (jnp.zeros((8, width), jnp.float32), zero, zero, zero) + (jnp.int32(0),) * 4
    carry = lax.fori_loop(0, 3, border, nothing)
    total, prod_z, w_lo, w_up, l1, r1, l2, r2 = lax.fori_loop(1, last - 1, inner, carry)
    total = total + lanes_store(l2, pl.multiple_of(r2, ROWS), w_lo, w_up)
    w_lo, w_up = lanes_weight(l1, pl.multiple_of(r1, ROWS), prod_z)
    total = total + lanes_store(l1, pl.multiple_of(r1, ROWS), w_lo, w_up)
    total = total + fold(grad[0, last - 1])
    total = total + jnp.where(has_lo, 0.0, 1.0) * fold(grad[0, 0]) + jnp.where(has_up, 0.0, 1.0) * fold(grad[0, last])
    def square(values):
        return values * values

    def face_top(rows, size):
        prod = jnp.zeros((size, width), jnp.float32)
        for t in range(steps):
            prod += (pa[steps + t, last, rows] - halo_t[steps + t, rows]) * (pa[t, last, rows] - halo_t[t, rows])
        k0, g_up = k[0, last, rows], halo_t[K, rows]
        w = weight(prod, pa[FACTOR, last, rows], k0, g_up)
        w_up = w * k0
        ret_t_out[rows] = w_up
        log0 = grad[0, last, rows] + w * g_up
        grad[0, last, rows] = log0
        return fold(log0), w_up

    def face_bottom(rows, size):
        prod = jnp.zeros((size, width), jnp.float32)
        for t in range(steps):
            prod += (halo_b[steps + t, rows] - pa[steps + t, 0, rows]) * (halo_b[t, rows] - pa[t, 0, rows])
        k0, g_up = halo_b[K, rows], pa[K, 0, rows]
        w = weight(prod, halo_b[FACTOR, rows], k0, g_up)
        w_lo = w * g_up
        ret_b_out[rows] = w_lo
        log0 = grad[0, 0, rows] + w * k0
        grad[0, 0, rows] = log0
        return fold(log0), w_lo

    def pair_face(b, total):
        squares, _ = face_top(pl.ds(pl.multiple_of(b * 32, 32), 32), 32)
        return total + squares

    @pl.when(even)
    def _():
        pair.wait_recv()

    total = lax.fori_loop(0, jnp.where(even, height // 32, 0), pair_face, total)

    @pl.when(even)
    def _():
        pair_back.start()

    def top_early(c, total):
        down(c, D, SEND).wait_recv()
        squares, _ = face_top(chunk_rows(c), CHUNK)
        back_up(c, BACK).start()
        return total + squares

    def top_late(c, total):
        down(c, DL, SEND_LATE).wait_recv()
        squares, w_up = face_top(chunk_rows(c), CHUNK)
        back_up(c, BACK_LATE).start()
        return total + squares + fold(halo_t[OWN_UP, chunk_rows(c)] + w_up)

    def bottom_early(c, total):
        up(c, U, SEND).wait_recv()
        squares, _ = face_bottom(chunk_rows(c), CHUNK)
        back_down(c, BACK).start()
        return total + squares

    def bottom_late(c, total):
        up(c, UL, SEND_LATE).wait_recv()
        squares, w_lo = face_bottom(chunk_rows(c), CHUNK)
        back_down(c, BACK_LATE).start()
        return total + squares + fold(halo_b[OWN_LO, chunk_rows(c)] + w_lo)

    def add_bottom(c, total):
        rows = chunk_rows(c)
        log0 = grad[0, 0, rows] + ret_b_in[rows]
        grad[0, 0, rows] = log0
        return total + fold(log0)

    def add_top(c, total):
        rows = chunk_rows(c)
        log0 = grad[0, last, rows] + ret_t_in[rows]
        grad[0, last, rows] = log0
        return total + fold(log0)

    def when_even(value):
        return jnp.where(even, value, 0)

    def when_odd(value):
        return jnp.where(odd, value, 0)

    @pl.when(odd)
    def _():
        pair_back.wait_recv()

    total = lax.fori_loop(0, when_odd(chunks), add_bottom, total)
    total = lax.fori_loop(0, when_odd(late_down), top_early, total)
    total = lax.fori_loop(when_even(share), when_even(late_up), bottom_early, total)
    for i in range(4, len(rounds) + 1):
        turn(i)
    each_share(even, lambda value, below, above: await_rows(ret_b_in, below, BACK))
    each_share(odd, lambda value, below, above: await_rows(ret_t_in, above - value, BACK))
    total = lax.fori_loop(0, when_even(late_down), add_bottom, total)
    total = lax.fori_loop(when_odd(share), when_odd(late_up), add_top, total)
    total = lax.fori_loop(when_odd(late_down), when_odd(share), top_late, total)
    total = lax.fori_loop(when_even(late_up), when_even(rows_end), bottom_late, total)

    mine = jnp.sum(total, axis=0, keepdims=True)
    part[...] = mine

    def to_peer(j):
        return pltpu.make_async_remote_copy(
            src_ref=part, dst_ref=parts.at[me], send_sem=sems.at[PART_SEND], recv_sem=sems.at[PART],
            device_id={"gx": j}, device_id_type=MESH)

    loop(0, me, lambda j: to_peer(j).start())
    loop(me + 1, n, lambda j: to_peer(j).start())
    parts[me] = mine

    each_share(even, lambda value, below, above: await_rows(ret_b_in, value - below, BACK_LATE))
    each_share(odd, lambda value, below, above: await_rows(ret_t_in, chunks - above, BACK_LATE))
    nowhere = jnp.zeros((8, width), jnp.float32)
    lax.fori_loop(when_even(late_down), when_even(share), add_bottom, nowhere)
    lax.fori_loop(when_odd(late_up), when_odd(rows_end), add_top, nowhere)

    def drain_even(value, below, above):
        await_planes_of(halo_t, D, below, SEND)
        await_planes_of(halo_t, DL, value - below, SEND_LATE)
        await_rows(ret_b_out, chunks - value, BACK_SEND)

    def drain_odd(value, below, above):
        await_planes_of(halo_b, U, above - value, SEND)
        await_planes_of(halo_b, UL, chunks - above, SEND_LATE)
        await_rows(ret_t_out, value, BACK_SEND)

    each_share(even, drain_even)
    each_share(odd, drain_odd)

    @pl.when(even)
    def _():
        pair_back.wait_send()

    @pl.when(odd)
    def _():
        pair.wait_send()

    others = parts.at[pl.ds(0, n - 1)]
    pltpu.make_async_copy(others, others, sems.at[PART_SEND]).wait()
    pltpu.make_async_copy(others, others, sems.at[PART]).wait()
    whole = jnp.sum(jnp.sum(parts[...], axis=0), keepdims=True)
    scale_out[...] = jnp.broadcast_to(lax.rsqrt(whole / entries + epsilon), scale_out.shape)


def finish(raw, scale, out, scaled, sem):
    dims, layers = raw.shape[:2]
    factor = jnp.broadcast_to(scale[0:1], raw.shape[2:])
    for d in range(dims):
        for l in range(layers):
            scaled[d, l] = raw[d, l] * factor
            pltpu.make_async_copy(scaled.at[d, l], out.at[d, l], sem.at[0]).start()
    pltpu.make_async_copy(scaled, out, sem.at[0]).wait()


def local(pressure, adjoint, permeability, active, fault_codes):
    n = lax.axis_size("gx")
    steps, layers, height, width = pressure.shape
    chunks = height // CHUNK
    f32 = jnp.float32
    padded = height + PAD
    dma = pltpu.SemaphoreType.DMA
    raw, scale = pl.pallas_call(
        functools.partial(kernel, n),
        out_shape=(pltpu.VMEM((3, layers, height, width), f32), pltpu.VMEM((8, width), f32)),
        in_specs=[pl.BlockSpec(memory_space=pltpu.HBM)] * 5,
        out_specs=(pl.BlockSpec(memory_space=pltpu.VMEM), pl.BlockSpec(memory_space=pltpu.VMEM)),
        scratch_shapes=[
            pltpu.VMEM((2 * steps + 3, layers, padded, width), f32),
            pltpu.VMEM((3, layers, padded, width), f32),
            pltpu.VMEM((layers, padded, width), jnp.int32),
            pltpu.VMEM((3, layers, height, width), jnp.int32),
            pltpu.VMEM((2 * steps + 2, height, width), f32),
            pltpu.VMEM((2 * steps + 3, height, width), f32),
            pltpu.VMEM((height, width), f32),
            pltpu.VMEM((height, width), f32),
            pltpu.VMEM((height, width), f32),
            pltpu.VMEM((height, width), f32),
            pltpu.VMEM((padded, width), f32),
            pltpu.VMEM((1, width), f32),
            pltpu.VMEM((n, 1, width), f32),
            dma((layers,)),
            dma((chunks,)),
            dma((10,)),
            pltpu.SemaphoreType.REGULAR((len(distances(n)),)),
        ],
        compiler_params=pltpu.CompilerParams(collective_id=0, has_side_effects=True, vmem_limit_bytes=GRANT),
        cost_estimate=pl.CostEstimate(flops=100_000_000, bytes_accessed=12_000_000, transcendentals=0),
        name="faces",
    )(pressure, adjoint, permeability, active, fault_codes)
    return pl.pallas_call(
        finish,
        out_shape=jax.ShapeDtypeStruct(raw.shape, f32),
        in_specs=[pl.BlockSpec(memory_space=pltpu.VMEM)] * 2,
        out_specs=pl.BlockSpec(memory_space=pltpu.HBM),
        scratch_shapes=[pltpu.VMEM((3, layers, height, width), f32), dma((1,))],
        compiler_params=pltpu.CompilerParams(vmem_limit_bytes=8_000_000),
        name="finish",
    )(raw, scale)


def solution(mesh):
    split = ("groups", "gx")
    placed = (P(None, split), P(None, split), P(None, split), P(split), P(None, split))
    return jax.shard_map(local, mesh=mesh, in_specs=placed, out_specs=P(None, split), check_vma=False)
```

```python
import functools

import jax
import jax.numpy as jnp
from jax import lax
from jax.experimental import pallas as pl
from jax.experimental.pallas import tpu as pltpu
from jax.sharding import PartitionSpec as P

MESH = pl.DeviceIdType.MESH
epsilon = 1e-06
ROWS = 64
CHUNK = 8
LATE = 4
HEAD = 2
PAD = 8
GRANT = 58_000_000


def doubled(codes):
    return jnp.where(codes == 0, 2.0, jnp.where(codes == 1, 1.2, jnp.where(codes == 2, 0.5, 0.1))).astype(jnp.float32)


def fold(values):
    squares = values * values
    total = squares[0:8]
    for i in range(8, squares.shape[0], 8):
        total = total + squares[i : i + 8]
    return total


def weight(products, factor, k_lo, k_up):
    summed = k_lo + k_up
    return factor * products * (k_lo * k_up) / jnp.maximum(summed * summed, 1e-30)


def distances(n):
    reach, rounds = 1, []
    while reach < n - 1:
        rounds.append(reach)
        reach *= 2
    return rounds


def down_shares(chips, chunks):
    rise = [(3 * chunks * q * q) // (4 * max(chips - 2, 1) ** 2) for q in range(chips - 1)]
    return [chunks - min(max(up, min(q, 1)), chunks) for q, up in enumerate(rise)]


def kernel(
    n, p_hbm, a_hbm, k_hbm, act_hbm, code_hbm, grad, scale_out,
    pa, k, act, code, halo_t, halo_b, ret_t_out, ret_b_out, ret_t_in, ret_b_in, tail, part, parts,
    load_sem, chunk_recv, sems, near_sem,
):
    me = lax.axis_index("gx")
    lower, upper = me - 1, me + 1
    steps, layers, height, width = p_hbm.shape
    last = layers - 1
    blocks = height // ROWS
    chunks = height // CHUNK
    entries = 3 * layers * n * height * width
    K, FACTOR = 2 * steps, 2 * steps + 1
    OWN_UP, OWN_LO = 2 * steps + 1, 2 * steps + 2
    SEND, SEND_LATE, BACK_SEND, BACK, BACK_LATE, PAIR_SEND, PAIR, PAIR_BACK, PART_SEND, PART = range(10)

    odd = me % 2
    even = odd == 0
    odd = odd == 1
    has_lo, has_up = me > 0, me < n - 1
    apart = jnp.where(even, me, n - 1 - me) > 0
    chip = (me + 1) // 2 - 1
    shares = down_shares(n // 2, chunks)
    share = jnp.int32(0)
    for q, value in enumerate(shares):
        share = jnp.where(chip == q, value, share)
    share = jnp.where(apart, share, 0)
    rows_end = jnp.where(apart, chunks, 0)
    late_down = jnp.where(share > LATE, share - LATE, 0)
    late_up = jnp.where(rows_end - LATE > share, rows_end - LATE, share)

    def loop(start, stop, body):
        def step(i, carry):
            body(i)
            return carry

        lax.fori_loop(start, stop, step, 0)

    barrier = pltpu.get_barrier_semaphore()

    def signal(semaphore, distance):
        for there, inside in ((me - distance, me >= distance), (me + distance, me + distance < n)):
            @pl.when(inside)
            def _():
                pl.semaphore_signal(semaphore, inc=1, device_id={"gx": there}, device_id_type=MESH)

    def await_signals(semaphore, distance):
        peers = jnp.where(me >= distance, 1, 0) + jnp.where(me + distance < n, 1, 0)
        pl.semaphore_wait(semaphore, peers)

    def fields(l, sem, start=0, stop=height):
        rows = pl.ds(start, stop - start)
        return (
            pltpu.make_async_copy(p_hbm.at[:, l, rows], pa.at[pl.ds(0, steps), l, rows], sem),
            pltpu.make_async_copy(a_hbm.at[:, l, rows], pa.at[pl.ds(steps, steps), l, rows], sem),
        )

    def k_of(start, stop, l, sem):
        axes = pl.ds(start, stop - start)
        return pltpu.make_async_copy(k_hbm.at[axes, l], k.at[axes, l, pl.ds(0, height)], sem)

    def code_of(start, stop, l, sem):
        axes = pl.ds(start, stop - start)
        return pltpu.make_async_copy(code_hbm.at[axes, l], code.at[axes, l], sem)

    def act_of(l, sem):
        return pltpu.make_async_copy(act_hbm.at[l], act.at[l, pl.ds(0, height)], sem)

    def cells(l, sem):
        return k_of(0, 3, l, sem), act_of(l, sem), code_of(0, 3, l, sem)

    head = HEAD * CHUNK
    load_k = pltpu.make_async_copy(k_hbm.at[0, last], pa.at[K, last, pl.ds(0, height)], load_sem.at[2])
    for copy in (
        (k_of(0, 1, 0, load_sem.at[0]), act_of(0, load_sem.at[0])) + fields(0, load_sem.at[0], 0, head)
        + fields(0, load_sem.at[1], head)
        + (load_k, act_of(last, load_sem.at[2]), code_of(0, 1, last, load_sem.at[2])) + fields(last, load_sem.at[2])
    ):
        copy.start()

    signal(barrier, 1)
    rounds = distances(n)

    def turn(i):
        if 0 < i <= len(rounds):
            await_signals(near_sem.at[i - 1], rounds[i - 1])
        if i < len(rounds):
            signal(near_sem.at[i], rounds[i])

    def start_layer(l, sem):
        for copy in fields(l, sem) + cells(l, sem):
            copy.start()

    def await_planes(planes, rank, sem, rows=height):
        ref = pa.at[pl.ds(0, planes), pl.ds(0, rank), pl.ds(0, rows)]
        pltpu.make_async_copy(ref, ref, sem).wait()

    def layer_sem(l):
        return load_sem.at[l + 2]


    def chunk_rows(c):
        return pl.ds(pl.multiple_of(c * CHUNK, CHUNK), CHUNK)

    def down(c, planes, kind):
        rows = chunk_rows(c)
        return pltpu.make_async_remote_copy(
            src_ref=pa.at[pl.ds(0, planes), 0, rows], dst_ref=halo_t.at[pl.ds(0, planes), rows],
            send_sem=sems.at[kind], recv_sem=chunk_recv.at[c], device_id={"gx": lower}, device_id_type=MESH)

    def up(c, planes, kind):
        rows = chunk_rows(c)
        return pltpu.make_async_remote_copy(
            src_ref=pa.at[pl.ds(0, planes), last, rows], dst_ref=halo_b.at[pl.ds(0, planes), rows],
            send_sem=sems.at[kind], recv_sem=chunk_recv.at[c], device_id={"gx": upper}, device_id_type=MESH)

    def back_up(c, kind):
        rows = chunk_rows(c)
        return pltpu.make_async_remote_copy(
            src_ref=ret_t_out.at[rows], dst_ref=ret_b_in.at[rows],
            send_sem=sems.at[BACK_SEND], recv_sem=sems.at[kind], device_id={"gx": upper}, device_id_type=MESH)

    def back_down(c, kind):
        rows = chunk_rows(c)
        return pltpu.make_async_remote_copy(
            src_ref=ret_b_out.at[rows], dst_ref=ret_t_in.at[rows],
            send_sem=sems.at[BACK_SEND], recv_sem=sems.at[kind], device_id={"gx": lower}, device_id_type=MESH)

    D, DL, U, UL = 2 * steps + 1, 2 * steps + 2, 2 * steps + 2, 2 * steps + 3

    pair = pltpu.make_async_remote_copy(
        src_ref=pa.at[pl.ds(0, D), 0, pl.ds(0, height)], dst_ref=halo_t.at[pl.ds(0, D)],
        send_sem=sems.at[PAIR_SEND], recv_sem=sems.at[PAIR], device_id={"gx": lower}, device_id_type=MESH)
    pair_back = pltpu.make_async_remote_copy(
        src_ref=ret_t_out, dst_ref=ret_b_in,
        send_sem=sems.at[PAIR_SEND], recv_sem=sems.at[PAIR_BACK], device_id={"gx": upper}, device_id_type=MESH)

    def await_bytes(ref, sem):
        pltpu.make_async_copy(ref, ref, sems.at[sem]).wait()

    def await_rows(ref, count, sem):
        if count > 0:
            await_bytes(ref.at[pl.ds(0, count * CHUNK)], sem)

    def await_planes_of(ref, planes, count, sem):
        if count > 0:
            await_bytes(ref.at[pl.ds(0, planes), pl.ds(0, count * CHUNK)], sem)

    def each_share(side, body):
        for value in sorted(set(shares)):
            @pl.when(jnp.logical_and(jnp.logical_and(apart, side), share == value))
            def _(value=value):
                body(value, max(value - LATE, 0), max(chunks - LATE, value))

    tail[0:8] = jnp.zeros((8, width), jnp.float32)

    def clear(l):
        for t in range(2 * steps):
            pa[t, l, height:] = jnp.zeros((PAD, width), jnp.float32)
        k[1, l, height:] = jnp.zeros((PAD, width), jnp.float32)
        act[l, height:] = jnp.zeros((PAD, width), jnp.int32)

    loop(0, layers, clear)

    await_signals(barrier, 1)
    await_planes(8, 1, load_sem.at[0], (2 * steps * head + 2 * height) // 8)
    pa[K, 0, 0:height] = k[0, 0, 0:height] * act[0, 0:height].astype(jnp.float32)
    ahead = jnp.where(late_down < HEAD, late_down, HEAD)

    @pl.when(even)
    def _():
        loop(0, ahead, lambda c: down(c, D, SEND).start())

    await_planes(2 * steps, 1, load_sem.at[1], height - head)

    @pl.when(even)
    def _():
        loop(ahead, late_down, lambda c: down(c, D, SEND).start())

    await_planes(2 * steps + 3, 1, load_sem.at[2])
    pa[FACTOR, last, 0:height] = doubled(code[0, last]) * act[last, 0:height].astype(jnp.float32)

    @pl.when(odd)
    def _():
        loop(share, late_up, lambda c: up(c, U, SEND).start())

    for copy in (
        k_of(1, 3, 0, load_sem.at[3]), code_of(0, 3, 0, load_sem.at[3]),
        k_of(0, 3, last, load_sem.at[3]), code_of(1, 3, last, load_sem.at[3]),
    ):
        copy.start()
    start_layer(1, load_sem.at[3])
    start_layer(last - 1, load_sem.at[3])
    loop(2, last - 1, lambda l: start_layer(l, layer_sem(l)))
    turn(0)

    zero = jnp.zeros((ROWS, width), jnp.float32)
    lane = lax.broadcasted_iota(jnp.int32, (ROWS, width), 1)
    for l in range(2, last - 1):
        grad[0, l] = jnp.zeros((height, width), jnp.float32)

    def opened(l, rows):
        return act[l, rows].astype(jnp.float32)

    def cross(l):
        def block(b):
            here = pl.ds(pl.multiple_of(b * ROWS, ROWS), ROWS)
            prod = zero
            for t in range(steps):
                prod += (pa[steps + t, l, here] - pa[steps + t, l + 1, here]) * (pa[t, l, here] - pa[t, l + 1, here])
            k0, k0_up = k[0, l, here] * opened(l, here), k[0, l + 1, here] * opened(l + 1, here)
            w = weight(prod, doubled(code[0, l, here]), k0, k0_up)
            grad[0, l, here] = w * k0_up
            grad[0, l + 1, here] = w * k0

        loop(0, blocks, block)

    await_planes(2 * steps - 1, 4, load_sem.at[3])
    cross(0)
    cross(last - 1)
    pa[OWN_UP, 0, 0:height] = grad[0, 0]
    pa[OWN_LO, last, 0:height] = grad[0, last]

    @pl.when(even)
    def _():
        loop(late_down, share, lambda c: down(c, DL, SEND_LATE).start())

    @pl.when(odd)
    def _():
        loop(late_up, rows_end, lambda c: up(c, UL, SEND_LATE).start())
        pair.start()

    turn(1)

    def lanes_weight(l, r, prod):
        here = pl.ds(r, ROWS)
        k2 = k[2, l, here] * opened(l, here)
        k2_up = jnp.where(lane < width - 1, pltpu.roll(k2, width - 1, 1), 0.0)
        w = weight(prod, doubled(code[2, l, here]), k2, k2_up)
        return w * k2_up, w * k2

    def lanes_store(l, r, w_lo, w_up):
        log2 = w_lo + pltpu.roll(w_up, 1, 1)
        grad[2, l, pl.ds(r, ROWS)] = log2
        return fold(log2)

    def layer(l, carry, crossing):
        def block(b, carry):
            total, prod_z, w_lo, w_up, l1, r1, l2, r2 = carry
            r = pl.multiple_of(b * ROWS, ROWS)
            here, after = pl.ds(r, ROWS), pl.ds(r + 1, ROWS)
            total = total + lanes_store(l2, pl.multiple_of(r2, ROWS), w_lo, w_up)
            w_lo, w_up = lanes_weight(l1, pl.multiple_of(r1, ROWS), prod_z)
            prod_x, prod_y, prod_z = zero, zero, zero
            for t in range(steps):
                pt, at = pa[t, l, here], pa[steps + t, l, here]
                prod_z += (at - pltpu.roll(at, width - 1, 1)) * (pt - pltpu.roll(pt, width - 1, 1))
                prod_y += (at - pa[steps + t, l, after]) * (pt - pa[t, l, after])
                if crossing:
                    prod_x += (at - pa[steps + t, l + 1, here]) * (pt - pa[t, l + 1, here])
            now = opened(l, here)
            k1, k1_up = k[1, l, here] * now, k[1, l, after] * opened(l, after)
            w = weight(prod_y, doubled(code[1, l, here]), k1, k1_up)
            tail[pl.ds(r + 8, ROWS)] = w * k1
            log1 = w * k1_up + tail[pl.ds(r + 7, ROWS)]
            grad[1, l, here] = log1
            total = total + fold(log1)
            if crossing:
                k0, k0_up = k[0, l, here] * now, k[0, l + 1, here] * opened(l + 1, here)
                w = weight(prod_x, doubled(code[0, l, here]), k0, k0_up)
                log0 = grad[0, l, here] + w * k0_up
                grad[0, l, here] = log0
                grad[0, l + 1, here] = grad[0, l + 1, here] + w * k0
                total = total + fold(log0)
            return total, prod_z, w_lo, w_up, l, r, l1, r1

        return lax.fori_loop(0, blocks, block, carry)

    def border(i, carry):
        return layer(jnp.where(i == 0, 0, last + 1 - i), carry, False)

    def inner(l, carry):
        @pl.when(l < last - 2)
        def _():
            await_planes(steps, 3, layer_sem(l + 1))

        for i, at_layer in ((2, 1), (3, last - 3)):
            @pl.when(l == at_layer)
            def _(i=i):
                turn(i)

        return layer(l, carry, True)

    nothing = (jnp.zeros((8, width), jnp.float32), zero, zero, zero) + (jnp.int32(0),) * 4
    carry = lax.fori_loop(0, 3, border, nothing)
    total, prod_z, w_lo, w_up, l1, r1, l2, r2 = lax.fori_loop(1, last - 1, inner, carry)
    total = total + lanes_store(l2, pl.multiple_of(r2, ROWS), w_lo, w_up)
    w_lo, w_up = lanes_weight(l1, pl.multiple_of(r1, ROWS), prod_z)
    total = total + lanes_store(l1, pl.multiple_of(r1, ROWS), w_lo, w_up)
    total = total + fold(grad[0, last - 1])
    total = total + jnp.where(has_lo, 0.0, 1.0) * fold(grad[0, 0]) + jnp.where(has_up, 0.0, 1.0) * fold(grad[0, last])
    def square(values):
        return values * values

    def face_top(rows, size):
        prod = jnp.zeros((size, width), jnp.float32)
        for t in range(steps):
            prod += (pa[steps + t, last, rows] - halo_t[steps + t, rows]) * (pa[t, last, rows] - halo_t[t, rows])
        k0, g_up = k[0, last, rows], halo_t[K, rows]
        w = weight(prod, pa[FACTOR, last, rows], k0, g_up)
        w_up = w * k0
        ret_t_out[rows] = w_up
        log0 = grad[0, last, rows] + w * g_up
        grad[0, last, rows] = log0
        return fold(log0), w_up

    def face_bottom(rows, size):
        prod = jnp.zeros((size, width), jnp.float32)
        for t in range(steps):
            prod += (halo_b[steps + t, rows] - pa[steps + t, 0, rows]) * (halo_b[t, rows] - pa[t, 0, rows])
        k0, g_up = halo_b[K, rows], pa[K, 0, rows]
        w = weight(prod, halo_b[FACTOR, rows], k0, g_up)
        w_lo = w * g_up
        ret_b_out[rows] = w_lo
        log0 = grad[0, 0, rows] + w * k0
        grad[0, 0, rows] = log0
        return fold(log0), w_lo

    def pair_face(b, total):
        squares, _ = face_top(pl.ds(pl.multiple_of(b * 32, 32), 32), 32)
        return total + squares

    @pl.when(even)
    def _():
        pair.wait_recv()

    total = lax.fori_loop(0, jnp.where(even, height // 32, 0), pair_face, total)

    @pl.when(even)
    def _():
        pair_back.start()

    def top_early(c, total):
        down(c, D, SEND).wait_recv()
        squares, _ = face_top(chunk_rows(c), CHUNK)
        back_up(c, BACK).start()
        return total + squares

    def top_late(c, total):
        down(c, DL, SEND_LATE).wait_recv()
        squares, w_up = face_top(chunk_rows(c), CHUNK)
        return total + squares + fold(halo_t[OWN_UP, chunk_rows(c)] + w_up)

    def bottom_early(c, total):
        up(c, U, SEND).wait_recv()
        squares, _ = face_bottom(chunk_rows(c), CHUNK)
        back_down(c, BACK).start()
        return total + squares

    def bottom_late(c, total):
        up(c, UL, SEND_LATE).wait_recv()
        squares, w_lo = face_bottom(chunk_rows(c), CHUNK)
        return total + squares + fold(halo_b[OWN_LO, chunk_rows(c)] + w_lo)

    def add_bottom(c, total):
        rows = chunk_rows(c)
        log0 = grad[0, 0, rows] + ret_b_in[rows]
        grad[0, 0, rows] = log0
        return total + fold(log0)

    def add_top(c, total):
        rows = chunk_rows(c)
        log0 = grad[0, last, rows] + ret_t_in[rows]
        grad[0, last, rows] = log0
        return total + fold(log0)

    def when_even(value):
        return jnp.where(even, value, 0)

    def when_odd(value):
        return jnp.where(odd, value, 0)

    @pl.when(odd)
    def _():
        pair_back.wait_recv()

    total = lax.fori_loop(0, when_odd(chunks), add_bottom, total)
    total = lax.fori_loop(0, when_odd(late_down), top_early, total)
    total = lax.fori_loop(when_even(share), when_even(late_up), bottom_early, total)
    for i in range(4, len(rounds) + 1):
        turn(i)
    each_share(even, lambda value, below, above: await_rows(ret_b_in, below, BACK))
    each_share(odd, lambda value, below, above: await_rows(ret_t_in, above - value, BACK))
    total = lax.fori_loop(0, when_even(late_down), add_bottom, total)
    total = lax.fori_loop(when_odd(share), when_odd(late_up), add_top, total)
    total = lax.fori_loop(when_odd(late_down), when_odd(share), top_late, total)
    total = lax.fori_loop(when_even(late_up), when_even(rows_end), bottom_late, total)

    mine = jnp.sum(total, axis=0, keepdims=True)
    part[...] = mine

    def to_peer(j):
        return pltpu.make_async_remote_copy(
            src_ref=part, dst_ref=parts.at[me], send_sem=sems.at[PART_SEND], recv_sem=sems.at[PART],
            device_id={"gx": j}, device_id_type=MESH)

    loop(0, me, lambda j: to_peer(j).start())
    loop(me + 1, n, lambda j: to_peer(j).start())
    loop(when_odd(late_down), when_odd(share), lambda c: back_up(c, BACK_LATE).start())
    loop(when_even(late_up), when_even(rows_end), lambda c: back_down(c, BACK_LATE).start())
    parts[me] = mine

    each_share(even, lambda value, below, above: await_rows(ret_b_in, value - below, BACK_LATE))
    each_share(odd, lambda value, below, above: await_rows(ret_t_in, chunks - above, BACK_LATE))
    nowhere = jnp.zeros((8, width), jnp.float32)
    lax.fori_loop(when_even(late_down), when_even(share), add_bottom, nowhere)
    lax.fori_loop(when_odd(late_up), when_odd(rows_end), add_top, nowhere)

    def drain_even(value, below, above):
        await_planes_of(halo_t, D, below, SEND)
        await_planes_of(halo_t, DL, value - below, SEND_LATE)
        await_rows(ret_b_out, chunks - value, BACK_SEND)

    def drain_odd(value, below, above):
        await_planes_of(halo_b, U, above - value, SEND)
        await_planes_of(halo_b, UL, chunks - above, SEND_LATE)
        await_rows(ret_t_out, value, BACK_SEND)

    each_share(even, drain_even)
    each_share(odd, drain_odd)

    @pl.when(even)
    def _():
        pair_back.wait_send()

    @pl.when(odd)
    def _():
        pair.wait_send()

    others = parts.at[pl.ds(0, n - 1)]
    pltpu.make_async_copy(others, others, sems.at[PART_SEND]).wait()
    pltpu.make_async_copy(others, others, sems.at[PART]).wait()
    whole = jnp.sum(jnp.sum(parts[...], axis=0), keepdims=True)
    scale_out[...] = jnp.broadcast_to(lax.rsqrt(whole / entries + epsilon), scale_out.shape)


def finish(raw, scale, out, scaled, sem):
    dims, layers = raw.shape[:2]
    factor = jnp.broadcast_to(scale[0:1], raw.shape[2:])
    for d in range(dims):
        for l in range(layers):
            scaled[d, l] = raw[d, l] * factor
            pltpu.make_async_copy(scaled.at[d, l], out.at[d, l], sem.at[0]).start()
    pltpu.make_async_copy(scaled, out, sem.at[0]).wait()


def local(pressure, adjoint, permeability, active, fault_codes):
    n = lax.axis_size("gx")
    steps, layers, height, width = pressure.shape
    chunks = height // CHUNK
    f32 = jnp.float32
    padded = height + PAD
    dma = pltpu.SemaphoreType.DMA
    raw, scale = pl.pallas_call(
        functools.partial(kernel, n),
        out_shape=(pltpu.VMEM((3, layers, height, width), f32), pltpu.VMEM((8, width), f32)),
        in_specs=[pl.BlockSpec(memory_space=pltpu.HBM)] * 5,
        out_specs=(pl.BlockSpec(memory_space=pltpu.VMEM), pl.BlockSpec(memory_space=pltpu.VMEM)),
        scratch_shapes=[
            pltpu.VMEM((2 * steps + 3, layers, padded, width), f32),
            pltpu.VMEM((3, layers, padded, width), f32),
            pltpu.VMEM((layers, padded, width), jnp.int32),
            pltpu.VMEM((3, layers, height, width), jnp.int32),
            pltpu.VMEM((2 * steps + 2, height, width), f32),
            pltpu.VMEM((2 * steps + 3, height, width), f32),
            pltpu.VMEM((height, width), f32),
            pltpu.VMEM((height, width), f32),
            pltpu.VMEM((height, width), f32),
            pltpu.VMEM((height, width), f32),
            pltpu.VMEM((padded, width), f32),
            pltpu.VMEM((1, width), f32),
            pltpu.VMEM((n, 1, width), f32),
            dma((layers,)),
            dma((chunks,)),
            dma((10,)),
            pltpu.SemaphoreType.REGULAR((len(distances(n)),)),
        ],
        compiler_params=pltpu.CompilerParams(collective_id=0, has_side_effects=True, vmem_limit_bytes=GRANT),
        cost_estimate=pl.CostEstimate(flops=100_000_000, bytes_accessed=12_000_000, transcendentals=0),
        name="faces",
    )(pressure, adjoint, permeability, active, fault_codes)
    return pl.pallas_call(
        finish,
        out_shape=jax.ShapeDtypeStruct(raw.shape, f32),
        in_specs=[pl.BlockSpec(memory_space=pltpu.VMEM)] * 2,
        out_specs=pl.BlockSpec(memory_space=pltpu.HBM),
        scratch_shapes=[pltpu.VMEM((3, layers, height, width), f32), dma((1,))],
        compiler_params=pltpu.CompilerParams(vmem_limit_bytes=8_000_000),
        name="finish",
    )(raw, scale)


def solution(mesh):
    split = ("groups", "gx")
    placed = (P(None, split), P(None, split), P(None, split), P(split), P(None, split))
    return jax.shard_map(local, mesh=mesh, in_specs=placed, out_specs=P(None, split), check_vma=False)
```

```python
import functools

import jax
import jax.numpy as jnp
from jax import lax
from jax.experimental import pallas as pl
from jax.experimental.pallas import tpu as pltpu
from jax.sharding import PartitionSpec as P

MESH = pl.DeviceIdType.MESH
epsilon = 1e-06
ROWS = 64
CHUNK = 8
LATE = 4
HEAD = 1
PAD = 8
GRANT = 58_000_000


def doubled(codes):
    return jnp.where(codes == 0, 2.0, jnp.where(codes == 1, 1.2, jnp.where(codes == 2, 0.5, 0.1))).astype(jnp.float32)


def fold(values):
    squares = values * values
    total = squares[0:8]
    for i in range(8, squares.shape[0], 8):
        total = total + squares[i : i + 8]
    return total


def weight(products, factor, k_lo, k_up):
    summed = k_lo + k_up
    return factor * products * (k_lo * k_up) / jnp.maximum(summed * summed, 1e-30)


def distances(n):
    reach, rounds = 1, []
    while reach < n - 1:
        rounds.append(reach)
        reach *= 2
    return rounds


def down_shares(chips, chunks):
    rise = [(3 * chunks * q * q) // (4 * max(chips - 2, 1) ** 2) for q in range(chips - 1)]
    return [chunks - min(max(up, min(q, 1)), chunks) for q, up in enumerate(rise)]


def kernel(
    n, p_hbm, a_hbm, k_hbm, act_hbm, code_hbm, grad, scale_out,
    pa, k, act, code, halo_t, halo_b, ret_t_out, ret_b_out, ret_t_in, ret_b_in, tail, part, parts,
    load_sem, chunk_recv, sems, near_sem,
):
    me = lax.axis_index("gx")
    lower, upper = me - 1, me + 1
    steps, layers, height, width = p_hbm.shape
    last = layers - 1
    blocks = height // ROWS
    chunks = height // CHUNK
    entries = 3 * layers * n * height * width
    K, FACTOR = 2 * steps, 2 * steps + 1
    OWN_UP, OWN_LO = 2 * steps + 1, 2 * steps + 2
    SEND, SEND_LATE, BACK_SEND, BACK, BACK_LATE, PAIR_SEND, PAIR, PAIR_BACK, PART_SEND, PART = range(10)

    odd = me % 2
    even = odd == 0
    odd = odd == 1
    has_lo, has_up = me > 0, me < n - 1
    apart = jnp.where(even, me, n - 1 - me) > 0
    chip = (me + 1) // 2 - 1
    shares = down_shares(n // 2, chunks)
    share = jnp.int32(0)
    for q, value in enumerate(shares):
        share = jnp.where(chip == q, value, share)
    share = jnp.where(apart, share, 0)
    rows_end = jnp.where(apart, chunks, 0)
    late_down = jnp.where(share > LATE, share - LATE, 0)
    late_up = jnp.where(rows_end - LATE > share, rows_end - LATE, share)

    def loop(start, stop, body):
        def step(i, carry):
            body(i)
            return carry

        lax.fori_loop(start, stop, step, 0)

    barrier = pltpu.get_barrier_semaphore()

    def signal(semaphore, distance):
        for there, inside in ((me - distance, me >= distance), (me + distance, me + distance < n)):
            @pl.when(inside)
            def _():
                pl.semaphore_signal(semaphore, inc=1, device_id={"gx": there}, device_id_type=MESH)

    def await_signals(semaphore, distance):
        peers = jnp.where(me >= distance, 1, 0) + jnp.where(me + distance < n, 1, 0)
        pl.semaphore_wait(semaphore, peers)

    def fields(l, sem, start=0, stop=height):
        rows = pl.ds(start, stop - start)
        return (
            pltpu.make_async_copy(p_hbm.at[:, l, rows], pa.at[pl.ds(0, steps), l, rows], sem),
            pltpu.make_async_copy(a_hbm.at[:, l, rows], pa.at[pl.ds(steps, steps), l, rows], sem),
        )

    def k_of(start, stop, l, sem):
        axes = pl.ds(start, stop - start)
        return pltpu.make_async_copy(k_hbm.at[axes, l], k.at[axes, l, pl.ds(0, height)], sem)

    def code_of(start, stop, l, sem):
        axes = pl.ds(start, stop - start)
        return pltpu.make_async_copy(code_hbm.at[axes, l], code.at[axes, l], sem)

    def act_of(l, sem):
        return pltpu.make_async_copy(act_hbm.at[l], act.at[l, pl.ds(0, height)], sem)

    def cells(l, sem):
        return k_of(0, 3, l, sem), act_of(l, sem), code_of(0, 3, l, sem)

    head = HEAD * CHUNK
    load_k = pltpu.make_async_copy(k_hbm.at[0, last], pa.at[K, last, pl.ds(0, height)], load_sem.at[2])
    for copy in (
        (k_of(0, 1, 0, load_sem.at[0]), act_of(0, load_sem.at[0])) + fields(0, load_sem.at[0], 0, head)
        + fields(0, load_sem.at[1], head)
        + (load_k, act_of(last, load_sem.at[2]), code_of(0, 1, last, load_sem.at[2])) + fields(last, load_sem.at[2])
    ):
        copy.start()

    signal(barrier, 1)
    rounds = distances(n)

    def turn(i):
        if 0 < i <= len(rounds):
            await_signals(near_sem.at[i - 1], rounds[i - 1])
        if i < len(rounds):
            signal(near_sem.at[i], rounds[i])

    def start_layer(l, sem):
        for copy in fields(l, sem) + cells(l, sem):
            copy.start()

    def await_planes(planes, rank, sem, rows=height):
        ref = pa.at[pl.ds(0, planes), pl.ds(0, rank), pl.ds(0, rows)]
        pltpu.make_async_copy(ref, ref, sem).wait()

    def layer_sem(l):
        return load_sem.at[l + 2]


    def chunk_rows(c):
        return pl.ds(pl.multiple_of(c * CHUNK, CHUNK), CHUNK)

    def down(c, planes, kind):
        rows = chunk_rows(c)
        return pltpu.make_async_remote_copy(
            src_ref=pa.at[pl.ds(0, planes), 0, rows], dst_ref=halo_t.at[pl.ds(0, planes), rows],
            send_sem=sems.at[kind], recv_sem=chunk_recv.at[c], device_id={"gx": lower}, device_id_type=MESH)

    def up(c, planes, kind):
        rows = chunk_rows(c)
        return pltpu.make_async_remote_copy(
            src_ref=pa.at[pl.ds(0, planes), last, rows], dst_ref=halo_b.at[pl.ds(0, planes), rows],
            send_sem=sems.at[kind], recv_sem=chunk_recv.at[c], device_id={"gx": upper}, device_id_type=MESH)

    def back_up(c, kind):
        rows = chunk_rows(c)
        return pltpu.make_async_remote_copy(
            src_ref=ret_t_out.at[rows], dst_ref=ret_b_in.at[rows],
            send_sem=sems.at[BACK_SEND], recv_sem=sems.at[kind], device_id={"gx": upper}, device_id_type=MESH)

    def back_down(c, kind):
        rows = chunk_rows(c)
        return pltpu.make_async_remote_copy(
            src_ref=ret_b_out.at[rows], dst_ref=ret_t_in.at[rows],
            send_sem=sems.at[BACK_SEND], recv_sem=sems.at[kind], device_id={"gx": lower}, device_id_type=MESH)

    D, DL, U, UL = 2 * steps + 1, 2 * steps + 2, 2 * steps + 2, 2 * steps + 3

    pair = pltpu.make_async_remote_copy(
        src_ref=pa.at[pl.ds(0, D), 0, pl.ds(0, height)], dst_ref=halo_t.at[pl.ds(0, D)],
        send_sem=sems.at[PAIR_SEND], recv_sem=sems.at[PAIR], device_id={"gx": lower}, device_id_type=MESH)
    pair_back = pltpu.make_async_remote_copy(
        src_ref=ret_t_out, dst_ref=ret_b_in,
        send_sem=sems.at[PAIR_SEND], recv_sem=sems.at[PAIR_BACK], device_id={"gx": upper}, device_id_type=MESH)

    def await_bytes(ref, sem):
        pltpu.make_async_copy(ref, ref, sems.at[sem]).wait()

    def await_rows(ref, count, sem):
        if count > 0:
            await_bytes(ref.at[pl.ds(0, count * CHUNK)], sem)

    def await_planes_of(ref, planes, count, sem):
        if count > 0:
            await_bytes(ref.at[pl.ds(0, planes), pl.ds(0, count * CHUNK)], sem)

    def each_share(side, body):
        for value in sorted(set(shares)):
            @pl.when(jnp.logical_and(jnp.logical_and(apart, side), share == value))
            def _(value=value):
                body(value, max(value - LATE, 0), max(chunks - LATE, value))

    tail[0:8] = jnp.zeros((8, width), jnp.float32)

    def clear(l):
        for t in range(2 * steps):
            pa[t, l, height:] = jnp.zeros((PAD, width), jnp.float32)
        k[1, l, height:] = jnp.zeros((PAD, width), jnp.float32)
        act[l, height:] = jnp.zeros((PAD, width), jnp.int32)

    loop(0, layers, clear)

    await_signals(barrier, 1)
    await_planes(8, 1, load_sem.at[0], (2 * steps * head + 2 * height) // 8)
    pa[K, 0, 0:head] = k[0, 0, 0:head] * act[0, 0:head].astype(jnp.float32)
    ahead = jnp.where(late_down < HEAD, late_down, HEAD)

    @pl.when(even)
    def _():
        loop(0, ahead, lambda c: down(c, D, SEND).start())

    pa[K, 0, head:height] = k[0, 0, head:height] * act[0, head:height].astype(jnp.float32)
    await_planes(2 * steps, 1, load_sem.at[1], height - head)

    @pl.when(even)
    def _():
        loop(ahead, late_down, lambda c: down(c, D, SEND).start())

    await_planes(2 * steps + 3, 1, load_sem.at[2])
    pa[FACTOR, last, 0:height] = doubled(code[0, last]) * act[last, 0:height].astype(jnp.float32)

    @pl.when(odd)
    def _():
        loop(share, late_up, lambda c: up(c, U, SEND).start())

    for copy in (
        k_of(1, 3, 0, load_sem.at[3]), code_of(0, 3, 0, load_sem.at[3]),
        k_of(0, 3, last, load_sem.at[3]), code_of(1, 3, last, load_sem.at[3]),
    ):
        copy.start()
    start_layer(1, load_sem.at[3])
    start_layer(last - 1, load_sem.at[3])
    loop(2, last - 1, lambda l: start_layer(l, layer_sem(l)))
    turn(0)

    zero = jnp.zeros((ROWS, width), jnp.float32)
    lane = lax.broadcasted_iota(jnp.int32, (ROWS, width), 1)
    for l in range(2, last - 1):
        grad[0, l] = jnp.zeros((height, width), jnp.float32)

    def opened(l, rows):
        return act[l, rows].astype(jnp.float32)

    def cross(l):
        def block(b):
            here = pl.ds(pl.multiple_of(b * ROWS, ROWS), ROWS)
            prod = zero
            for t in range(steps):
                prod += (pa[steps + t, l, here] - pa[steps + t, l + 1, here]) * (pa[t, l, here] - pa[t, l + 1, here])
            k0, k0_up = k[0, l, here] * opened(l, here), k[0, l + 1, here] * opened(l + 1, here)
            w = weight(prod, doubled(code[0, l, here]), k0, k0_up)
            grad[0, l, here] = w * k0_up
            grad[0, l + 1, here] = w * k0

        loop(0, blocks, block)

    await_planes(2 * steps - 1, 4, load_sem.at[3])
    cross(0)
    cross(last - 1)
    pa[OWN_UP, 0, 0:height] = grad[0, 0]
    pa[OWN_LO, last, 0:height] = grad[0, last]

    @pl.when(even)
    def _():
        loop(late_down, share, lambda c: down(c, DL, SEND_LATE).start())

    @pl.when(odd)
    def _():
        loop(late_up, rows_end, lambda c: up(c, UL, SEND_LATE).start())
        pair.start()

    turn(1)

    def lanes_weight(l, r, prod):
        here = pl.ds(r, ROWS)
        k2 = k[2, l, here] * opened(l, here)
        k2_up = jnp.where(lane < width - 1, pltpu.roll(k2, width - 1, 1), 0.0)
        w = weight(prod, doubled(code[2, l, here]), k2, k2_up)
        return w * k2_up, w * k2

    def lanes_store(l, r, w_lo, w_up):
        log2 = w_lo + pltpu.roll(w_up, 1, 1)
        grad[2, l, pl.ds(r, ROWS)] = log2
        return fold(log2)

    def layer(l, carry, crossing):
        def block(b, carry):
            total, prod_z, w_lo, w_up, l1, r1, l2, r2 = carry
            r = pl.multiple_of(b * ROWS, ROWS)
            here, after = pl.ds(r, ROWS), pl.ds(r + 1, ROWS)
            total = total + lanes_store(l2, pl.multiple_of(r2, ROWS), w_lo, w_up)
            w_lo, w_up = lanes_weight(l1, pl.multiple_of(r1, ROWS), prod_z)
            prod_x, prod_y, prod_z = zero, zero, zero
            for t in range(steps):
                pt, at = pa[t, l, here], pa[steps + t, l, here]
                prod_z += (at - pltpu.roll(at, width - 1, 1)) * (pt - pltpu.roll(pt, width - 1, 1))
                prod_y += (at - pa[steps + t, l, after]) * (pt - pa[t, l, after])
                if crossing:
                    prod_x += (at - pa[steps + t, l + 1, here]) * (pt - pa[t, l + 1, here])
            now = opened(l, here)
            k1, k1_up = k[1, l, here] * now, k[1, l, after] * opened(l, after)
            w = weight(prod_y, doubled(code[1, l, here]), k1, k1_up)
            tail[pl.ds(r + 8, ROWS)] = w * k1
            log1 = w * k1_up + tail[pl.ds(r + 7, ROWS)]
            grad[1, l, here] = log1
            total = total + fold(log1)
            if crossing:
                k0, k0_up = k[0, l, here] * now, k[0, l + 1, here] * opened(l + 1, here)
                w = weight(prod_x, doubled(code[0, l, here]), k0, k0_up)
                log0 = grad[0, l, here] + w * k0_up
                grad[0, l, here] = log0
                grad[0, l + 1, here] = grad[0, l + 1, here] + w * k0
                total = total + fold(log0)
            return total, prod_z, w_lo, w_up, l, r, l1, r1

        return lax.fori_loop(0, blocks, block, carry)

    def border(i, carry):
        return layer(jnp.where(i == 0, 0, last + 1 - i), carry, False)

    def inner(l, carry):
        @pl.when(l < last - 2)
        def _():
            await_planes(steps, 3, layer_sem(l + 1))

        for i, at_layer in ((2, 1), (3, last - 3)):
            @pl.when(l == at_layer)
            def _(i=i):
                turn(i)

        return layer(l, carry, True)

    nothing = (jnp.zeros((8, width), jnp.float32), zero, zero, zero) + (jnp.int32(0),) * 4
    carry = lax.fori_loop(0, 3, border, nothing)
    total, prod_z, w_lo, w_up, l1, r1, l2, r2 = lax.fori_loop(1, last - 1, inner, carry)
    total = total + lanes_store(l2, pl.multiple_of(r2, ROWS), w_lo, w_up)
    w_lo, w_up = lanes_weight(l1, pl.multiple_of(r1, ROWS), prod_z)
    total = total + lanes_store(l1, pl.multiple_of(r1, ROWS), w_lo, w_up)
    total = total + fold(grad[0, last - 1])
    total = total + jnp.where(has_lo, 0.0, 1.0) * fold(grad[0, 0]) + jnp.where(has_up, 0.0, 1.0) * fold(grad[0, last])
    def square(values):
        return values * values

    def face_top(rows, size):
        prod = jnp.zeros((size, width), jnp.float32)
        for t in range(steps):
            prod += (pa[steps + t, last, rows] - halo_t[steps + t, rows]) * (pa[t, last, rows] - halo_t[t, rows])
        k0, g_up = k[0, last, rows], halo_t[K, rows]
        w = weight(prod, pa[FACTOR, last, rows], k0, g_up)
        w_up = w * k0
        ret_t_out[rows] = w_up
        log0 = grad[0, last, rows] + w * g_up
        grad[0, last, rows] = log0
        return fold(log0), w_up

    def face_bottom(rows, size):
        prod = jnp.zeros((size, width), jnp.float32)
        for t in range(steps):
            prod += (halo_b[steps + t, rows] - pa[steps + t, 0, rows]) * (halo_b[t, rows] - pa[t, 0, rows])
        k0, g_up = halo_b[K, rows], pa[K, 0, rows]
        w = weight(prod, halo_b[FACTOR, rows], k0, g_up)
        w_lo = w * g_up
        ret_b_out[rows] = w_lo
        log0 = grad[0, 0, rows] + w * k0
        grad[0, 0, rows] = log0
        return fold(log0), w_lo

    def pair_face(b, total):
        squares, _ = face_top(pl.ds(pl.multiple_of(b * 32, 32), 32), 32)
        return total + squares

    @pl.when(even)
    def _():
        pair.wait_recv()

    total = lax.fori_loop(0, jnp.where(even, height // 32, 0), pair_face, total)

    @pl.when(even)
    def _():
        pair_back.start()

    def top_early(c, total):
        down(c, D, SEND).wait_recv()
        squares, _ = face_top(chunk_rows(c), CHUNK)
        back_up(c, BACK).start()
        return total + squares

    def top_late(c, total):
        down(c, DL, SEND_LATE).wait_recv()
        squares, w_up = face_top(chunk_rows(c), CHUNK)
        return total + squares + fold(halo_t[OWN_UP, chunk_rows(c)] + w_up)

    def bottom_early(c, total):
        up(c, U, SEND).wait_recv()
        squares, _ = face_bottom(chunk_rows(c), CHUNK)
        back_down(c, BACK).start()
        return total + squares

    def bottom_late(c, total):
        up(c, UL, SEND_LATE).wait_recv()
        squares, w_lo = face_bottom(chunk_rows(c), CHUNK)
        return total + squares + fold(halo_b[OWN_LO, chunk_rows(c)] + w_lo)

    def add_bottom(c, total):
        rows = chunk_rows(c)
        log0 = grad[0, 0, rows] + ret_b_in[rows]
        grad[0, 0, rows] = log0
        return total + fold(log0)

    def add_top(c, total):
        rows = chunk_rows(c)
        log0 = grad[0, last, rows] + ret_t_in[rows]
        grad[0, last, rows] = log0
        return total + fold(log0)

    def when_even(value):
        return jnp.where(even, value, 0)

    def when_odd(value):
        return jnp.where(odd, value, 0)

    @pl.when(odd)
    def _():
        pair_back.wait_recv()

    total = lax.fori_loop(0, when_odd(chunks), add_bottom, total)
    total = lax.fori_loop(0, when_odd(late_down), top_early, total)
    total = lax.fori_loop(when_even(share), when_even(late_up), bottom_early, total)
    for i in range(4, len(rounds) + 1):
        turn(i)
    each_share(even, lambda value, below, above: await_rows(ret_b_in, below, BACK))
    each_share(odd, lambda value, below, above: await_rows(ret_t_in, above - value, BACK))
    total = lax.fori_loop(0, when_even(late_down), add_bottom, total)
    total = lax.fori_loop(when_odd(share), when_odd(late_up), add_top, total)
    total = lax.fori_loop(when_odd(late_down), when_odd(share), top_late, total)
    total = lax.fori_loop(when_even(late_up), when_even(rows_end), bottom_late, total)

    mine = jnp.sum(total, axis=0, keepdims=True)
    part[...] = mine

    def to_peer(j):
        return pltpu.make_async_remote_copy(
            src_ref=part, dst_ref=parts.at[me], send_sem=sems.at[PART_SEND], recv_sem=sems.at[PART],
            device_id={"gx": j}, device_id_type=MESH)

    loop(0, me, lambda j: to_peer(j).start())
    loop(me + 1, n, lambda j: to_peer(j).start())
    loop(when_odd(late_down), when_odd(share), lambda c: back_up(c, BACK_LATE).start())
    loop(when_even(late_up), when_even(rows_end), lambda c: back_down(c, BACK_LATE).start())
    parts[me] = mine

    each_share(even, lambda value, below, above: await_rows(ret_b_in, value - below, BACK_LATE))
    each_share(odd, lambda value, below, above: await_rows(ret_t_in, chunks - above, BACK_LATE))
    nowhere = jnp.zeros((8, width), jnp.float32)
    lax.fori_loop(when_even(late_down), when_even(share), add_bottom, nowhere)
    lax.fori_loop(when_odd(late_up), when_odd(rows_end), add_top, nowhere)

    def drain_even(value, below, above):
        await_planes_of(halo_t, D, below, SEND)
        await_planes_of(halo_t, DL, value - below, SEND_LATE)
        await_rows(ret_b_out, chunks - value, BACK_SEND)

    def drain_odd(value, below, above):
        await_planes_of(halo_b, U, above - value, SEND)
        await_planes_of(halo_b, UL, chunks - above, SEND_LATE)
        await_rows(ret_t_out, value, BACK_SEND)

    each_share(even, drain_even)
    each_share(odd, drain_odd)

    @pl.when(even)
    def _():
        pair_back.wait_send()

    @pl.when(odd)
    def _():
        pair.wait_send()

    others = parts.at[pl.ds(0, n - 1)]
    pltpu.make_async_copy(others, others, sems.at[PART_SEND]).wait()
    pltpu.make_async_copy(others, others, sems.at[PART]).wait()
    whole = jnp.sum(jnp.sum(parts[...], axis=0), keepdims=True)
    scale_out[...] = jnp.broadcast_to(lax.rsqrt(whole / entries + epsilon), scale_out.shape)


def finish(raw, scale, out, scaled, sem):
    dims, layers = raw.shape[:2]
    factor = jnp.broadcast_to(scale[0:1], raw.shape[2:])
    for d in range(dims):
        for l in range(layers):
            scaled[d, l] = raw[d, l] * factor
            pltpu.make_async_copy(scaled.at[d, l], out.at[d, l], sem.at[0]).start()
    pltpu.make_async_copy(scaled, out, sem.at[0]).wait()


def local(pressure, adjoint, permeability, active, fault_codes):
    n = lax.axis_size("gx")
    steps, layers, height, width = pressure.shape
    chunks = height // CHUNK
    f32 = jnp.float32
    padded = height + PAD
    dma = pltpu.SemaphoreType.DMA
    raw, scale = pl.pallas_call(
        functools.partial(kernel, n),
        out_shape=(pltpu.VMEM((3, layers, height, width), f32), pltpu.VMEM((8, width), f32)),
        in_specs=[pl.BlockSpec(memory_space=pltpu.HBM)] * 5,
        out_specs=(pl.BlockSpec(memory_space=pltpu.VMEM), pl.BlockSpec(memory_space=pltpu.VMEM)),
        scratch_shapes=[
            pltpu.VMEM((2 * steps + 3, layers, padded, width), f32),
            pltpu.VMEM((3, layers, padded, width), f32),
            pltpu.VMEM((layers, padded, width), jnp.int32),
            pltpu.VMEM((3, layers, height, width), jnp.int32),
            pltpu.VMEM((2 * steps + 2, height, width), f32),
            pltpu.VMEM((2 * steps + 3, height, width), f32),
            pltpu.VMEM((height, width), f32),
            pltpu.VMEM((height, width), f32),
            pltpu.VMEM((height, width), f32),
            pltpu.VMEM((height, width), f32),
            pltpu.VMEM((padded, width), f32),
            pltpu.VMEM((1, width), f32),
            pltpu.VMEM((n, 1, width), f32),
            dma((layers,)),
            dma((chunks,)),
            dma((10,)),
            pltpu.SemaphoreType.REGULAR((len(distances(n)),)),
        ],
        compiler_params=pltpu.CompilerParams(collective_id=0, has_side_effects=True, vmem_limit_bytes=GRANT),
        cost_estimate=pl.CostEstimate(flops=100_000_000, bytes_accessed=12_000_000, transcendentals=0),
        name="faces",
    )(pressure, adjoint, permeability, active, fault_codes)
    return pl.pallas_call(
        finish,
        out_shape=jax.ShapeDtypeStruct(raw.shape, f32),
        in_specs=[pl.BlockSpec(memory_space=pltpu.VMEM)] * 2,
        out_specs=pl.BlockSpec(memory_space=pltpu.HBM),
        scratch_shapes=[pltpu.VMEM((3, layers, height, width), f32), dma((1,))],
        compiler_params=pltpu.CompilerParams(vmem_limit_bytes=8_000_000),
        name="finish",
    )(raw, scale)


def solution(mesh):
    split = ("groups", "gx")
    placed = (P(None, split), P(None, split), P(None, split), P(split), P(None, split))
    return jax.shard_map(local, mesh=mesh, in_specs=placed, out_specs=P(None, split), check_vma=False)
```
